32 devices in a mesh: au: 2 (over y), ia: 16 (over z, x, core).
Axes of the slice: x: 2, y: 2, z: 4, core: 2. Of those that a mesh axis runs over, the one named last changes fastest.
Arguments:
- user_factors: bfloat16 [1024, 256], P(('au', 'ia')), may hold values from -6 to 6
- item_factors: bfloat16 [16384, 256], P(('ia', 'au')), may hold values from -6 to 6
- user_tangent: bfloat16 [1024, 256], P(('au', 'ia')), may hold values from -6 to 6
- item_tangent: bfloat16 [16384, 256], P(('ia', 'au')), may hold values from -6 to 6
- block_mask: int32 [8, 128], P('au', 'ia'), may hold values from 0 to 1, as said below
Outputs:
- user_product: float32 [1024, 256], P(('au', 'ia'))
- item_product: float32 [16384, 256], P(('ia', 'au'))
The draws below stay inside these ranges and needn't reach their ends.
Inputs may be any that keep to these rules, and one draw needn't show every extreme that they name: `block_mask`: users are grouped in runs of 32 * 16 and items in runs of 512 * 2; where one user group meets one item group, at most 16 of its 4 x 8 blocks are observed, and in every draw one such meeting has exactly 16.
All inputs are finite; a program needn't handle non-finite values.
Results may differ from the reference program's by a relative error of at most 0.0013.
Values may be sent and summed in bfloat16 or wider, within the bound.
No kernel may reach another device: no remote copies, remote signals or barrier semaphores. Data moves between devices by JAX's collectives and lax.ppermute only.
A program may use at most 64 MiB of HBM per device.

```python
import jax
import jax.numpy as jnp
from jax import lax

R = 256
US_DEV = 32
IT_DEV = 512
USERS = 1024
ITEMS = 16384
ROWBLK = 4
COLBLK = 8
UBLK = 8
IBLK = 128
MAXB = 16
N_AU = 2
N_IA = 16


def draw_block_mask(key, part):
    key_count = jax.random.fold_in(key, 11)
    key_heavy = jax.random.fold_in(key, 12)
    key_place = jax.random.fold_in(key, 13)
    regions = N_AU * N_IA
    region_size = ROWBLK * COLBLK
    counts = jax.random.randint(key_count, (regions,), MAXB // 8, MAXB * 7 // 8 + 1)
    heavy = jax.random.randint(key_heavy, (), 0, regions)
    counts = jnp.where(jnp.arange(regions) == heavy, MAXB, counts)
    region_keys = jax.random.split(key_place, regions)
    places = jax.vmap(lambda k: jax.random.permutation(k, region_size))(region_keys)
    marks = (places < counts[:, None]).astype(jnp.int32)
    marks = marks.reshape(N_AU, N_IA, ROWBLK, COLBLK)
    marks = jnp.transpose(marks, (0, 2, 1, 3))
    return marks.reshape(UBLK, IBLK)


def block_scale(rng, shape, cuts, smallest, largest):
    level = 1.0
    for dim, blocks in cuts:
        steps = jax.random.uniform(jax.random.fold_in(jax.random.fold_in(rng, 6), dim), (blocks,), jnp.float32, smallest / len(cuts), largest / len(cuts))
        level = level * jnp.repeat(jnp.exp(steps), shape[dim] // blocks).reshape((-1,) + (1,) * (len(shape) - 1 - dim))
    return level


def bell_draw(own_key, extent, scale, limit, pieces=(), kind=jnp.bfloat16):
    loudness = block_scale(own_key, extent, pieces, -0.22, 0.18) if pieces else 1.0
    entries = jax.random.normal(own_key, extent, jnp.float32) * scale * loudness
    return jnp.minimum(jnp.maximum(entries, -limit), limit).astype(kind)


def setup_inputs(seed: int = 0) -> dict:
    splits = jax.random.split(jax.random.key(seed), 6)
    return {
        "user_factors": bell_draw(splits[0], (USERS, R), 1.0, 6.0, ((0, 32),)),
        "item_factors": bell_draw(splits[1], (ITEMS, R), 1.0, 6.0, ((0, 32),)),
        "user_tangent": bell_draw(splits[2], (USERS, R), 1.0, 6.0, ((0, 32),)),
        "item_tangent": bell_draw(splits[3], (ITEMS, R), 1.0, 6.0, ((0, 32),)),
        "block_mask": draw_block_mask(jax.random.fold_in(splits[5], 71), 0),
    }


batch_blocks = 16

def region_pass(users, user_tan, items, item_tan, mask_part):
    row_blocks, col_blocks = mask_part.shape
    block_rows = users.shape[0] // row_blocks
    width = users.shape[1]
    user_tiles = users.reshape(row_blocks, block_rows, width)
    utan_tiles = user_tan.reshape(row_blocks, block_rows, width)
    item_tiles = items.reshape(col_blocks, block_rows, width)
    itan_tiles = item_tan.reshape(col_blocks, block_rows, width)
    total = row_blocks * col_blocks
    flat = mask_part.reshape(-1).astype(jnp.int32)
    index = jnp.arange(total, dtype=jnp.int32)
    order = jnp.argsort((1 - flat) * total + index).astype(jnp.int32)
    live = flat[order].astype(jnp.float32)
    order = jnp.concatenate([order, jnp.zeros((batch_blocks,), jnp.int32)])
    live = jnp.concatenate([live, jnp.zeros((batch_blocks,), jnp.float32)])
    row_ids = (order // col_blocks).astype(jnp.int32)
    col_ids = (order % col_blocks).astype(jnp.int32)
    scaling = 1.0 / jnp.sqrt(jnp.float32(width))
    turns = -(-total // batch_blocks)

    def one_turn(turn, carry):
        acc_user, acc_item = carry
        first = (turn * batch_blocks).astype(jnp.int32)
        rsel = lax.dynamic_slice_in_dim(row_ids, first, batch_blocks)
        csel = lax.dynamic_slice_in_dim(col_ids, first, batch_blocks)
        lsel = lax.dynamic_slice_in_dim(live, first, batch_blocks)
        urow = user_tiles[rsel].astype(jnp.float32)
        durow = utan_tiles[rsel].astype(jnp.float32)
        vrow = item_tiles[csel].astype(jnp.float32)
        dvrow = itan_tiles[csel].astype(jnp.float32)
        score = jnp.einsum('gar,gbr->gab', urow, vrow) * scaling
        prob = jax.nn.sigmoid(score)
        weight = prob * (1.0 - prob)
        tang = (jnp.einsum('gar,gbr->gab', durow, vrow) + jnp.einsum('gar,gbr->gab', urow, dvrow)) * scaling
        curv = (lsel[:, None, None] * weight * tang).astype(jnp.bfloat16).astype(jnp.float32)
        to_user = jnp.einsum('gab,gbr->gar', curv, vrow)
        to_item = jnp.einsum('gab,gar->gbr', curv, urow)
        onehot_rows = (rsel[:, None] == jnp.arange(row_blocks, dtype=jnp.int32)[None, :]).astype(jnp.float32)
        onehot_cols = (csel[:, None] == jnp.arange(col_blocks, dtype=jnp.int32)[None, :]).astype(jnp.float32)
        acc_user = acc_user + jnp.einsum('gk,gar->kar', onehot_rows, to_user, precision=lax.Precision.HIGHEST)
        acc_item = acc_item + jnp.einsum('gk,gbr->kbr', onehot_cols, to_item, precision=lax.Precision.HIGHEST)
        return (acc_user, acc_item)
    start = (jnp.zeros((row_blocks, block_rows, width), jnp.float32), jnp.zeros((col_blocks, block_rows, width), jnp.float32))
    acc_user, acc_item = lax.fori_loop(0, turns, one_turn, start)
    return ((acc_user * scaling).reshape(-1, width), (acc_item * scaling).reshape(-1, width))

def reference(user_factors, item_factors, user_tangent, item_tangent, block_mask):
    group_rows = US_DEV * N_IA
    column_rows = IT_DEV * N_AU

    def per_group(carry, group):
        users = lax.dynamic_slice_in_dim(user_factors, group * group_rows, group_rows, 0)
        user_tan = lax.dynamic_slice_in_dim(user_tangent, group * group_rows, group_rows, 0)
        masks = lax.dynamic_slice_in_dim(block_mask, group * ROWBLK, ROWBLK, 0)

        def per_column(column):
            items = lax.dynamic_slice_in_dim(item_factors, column * column_rows, column_rows, 0)
            item_tan = lax.dynamic_slice_in_dim(item_tangent, column * column_rows, column_rows, 0)
            mask_part = lax.dynamic_slice_in_dim(masks, column * COLBLK, COLBLK, 1)
            return region_pass(users, user_tan, items, item_tan, mask_part)
        part_user, part_item = lax.map(per_column, jnp.arange(N_IA, dtype=jnp.int32))
        return (carry + part_item.reshape(ITEMS, R), lax.optimization_barrier(jnp.sum(part_user, axis=0)))
    item_total, user_parts = lax.scan(per_group, jnp.zeros((ITEMS, R), jnp.float32), jnp.arange(N_AU, dtype=jnp.int32))
    return (user_parts.reshape(USERS, R), item_total)
```

```python
import functools
import math

import jax
import jax.numpy as jnp
from jax import lax
from jax.experimental import pallas as pl
from jax.experimental.pallas import tpu as pltpu
from jax.sharding import PartitionSpec as P

f32 = jnp.float32
bf16 = jnp.bfloat16
NN = (((1,), (0,)), ((), ()))
NT = (((1,), (1,)), ((), ()))
TN = (((0,), (0,)), ((), ()))
dot = functools.partial(lax.dot_general, preferred_element_type=f32)


def swap(x, axis, size, bit):
    return lax.ppermute(x, axis, [(i, i ^ bit) for i in range(size)])


def bits_of(low, high):
    out = []
    bit = high // 2
    while bit >= low:
        out.append(bit)
        bit //= 2
    return out


def relative(bits):
    order = [0]
    for bit in bits:
        order = order + [r ^ bit for r in order]
    return order


def gather_pieces(own, axis, size, bits):
    pieces = [own[None]]
    for bit in bits:
        held = pieces[0] if len(pieces) == 1 else jnp.concatenate(pieces, 0)
        pieces.append(swap(held, axis, size, bit))
    return pieces


def region_kernel(*refs, n_groups, n_items, rel_rows, rel_items, scale):
    mask = refs[0]
    users = refs[1 : 1 + n_groups]
    at = 1 + n_groups
    items = refs[at : at + n_items]
    at += n_items
    tans = refs[at : at + n_items]
    at += n_items
    keep, send = refs[at : at + 2]
    at += 2
    outs = refs[at : at + n_items]
    at += n_items
    u_all, c_all = refs[at : at + 2]

    n_rb, _, us, width = users[0].shape[1:]
    members = 2 * send.shape[0]
    block = members * us
    me_rb = lax.axis_index("ia") // members
    me_au = lax.axis_index("au")
    m = 0
    for ref in users:
        for k in range(ref.shape[0]):
            u_all[:, :, pl.ds(m * us, us), :] = ref[k]
            m += 1
    it_dev = items[0].shape[1]
    cpd = it_dev // block
    pair = 2
    first = True
    for rp in range(n_rb // pair):
        fac = u_all[pl.ds(pair * rp, pair), 0].reshape(pair * block, width)
        tan = u_all[pl.ds(pair * rp, pair), 1].reshape(pair * block, width)
        total = None
        q = 0
        for g in range(n_items):
            for k in range(items[g].shape[0]):
                for ib in range(cpd // pair):
                    rows = pl.ds(ib * pair * block, pair * block)
                    v = items[g][k, rows, :]
                    dv = tans[g][k, rows, :]
                    s = dot(v, fac, NT)
                    t = dot(v, tan, NT) + dot(dv, fac, NT)
                    seen = jnp.concatenate(
                        [
                            jnp.concatenate(
                                [
                                    jnp.full(
                                        (block, block),
                                        mask[me_rb ^ rel_rows[pair * rp + j], (me_au ^ rel_items[q]) * cpd + pair * ib + i].astype(f32)
                                        * scale,
                                        f32,
                                    )
                                    for j in range(pair)
                                ],
                                1,
                            )
                            for i in range(pair)
                        ],
                        0,
                    )
                    e = jnp.exp(jnp.abs(s) * -scale)
                    p = 1.0 / (1.0 + e)
                    c = (e * p * p * (t * seen)).astype(bf16)
                    c_all[rows, :] = c
                    r = dot(c, fac, NN) * scale
                    if rp == 0:
                        outs[g][k, rows, :] = r
                    else:
                        outs[g][k, rows, :] += r
                part = dot(c_all[...], items[g][k], TN)
                total = part if total is None else total + part
                q += 1
        total = (total * scale).reshape(pair, members, us, width)
        half = members // 2
        for j in range(pair):
            for x in range(half):
                keep[x, pair * rp + j] = total[j, x]
                send[x, pair * rp + j] = total[j, half + x]


def on_device(user_factors, item_factors, user_tangent, item_tangent, block_mask, n_au, n_ia):
    us, width = user_factors.shape
    it = item_factors.shape[0]
    row_blocks, col_blocks = block_mask.shape
    block = us * n_ia // row_blocks
    members = block // us
    scale = 1.0 / math.sqrt(width)

    item_bits = bits_of(1, n_au)
    vs = gather_pieces(item_factors, "au", n_au, item_bits)
    dvs = gather_pieces(item_tangent, "au", n_au, item_bits)

    users = jnp.stack([user_factors, user_tangent])[None]
    row_bits = bits_of(members, n_ia)
    for bit in row_bits:
        users = jnp.concatenate([users, swap(users, "ia", n_ia, bit)], 0)
    pieces = gather_pieces(users, "ia", n_ia, bits_of(1, members))

    vm = pl.BlockSpec(memory_space=pltpu.VMEM)
    outs = pl.pallas_call(
        functools.partial(
            region_kernel,
            n_groups=len(pieces),
            n_items=len(vs),
            rel_rows=[r // members for r in relative(row_bits)],
            rel_items=relative(item_bits),
            scale=scale,
        ),
        in_specs=[pl.BlockSpec(memory_space=pltpu.SMEM)] + [vm] * (len(pieces) + 2 * len(vs)),
        out_specs=[vm] * (2 + len(vs)),
        out_shape=[
            jax.ShapeDtypeStruct((members // 2, row_blocks, us, width), f32),
            jax.ShapeDtypeStruct((members // 2, row_blocks, us, width), f32),
        ]
        + [jax.ShapeDtypeStruct(v.shape, f32) for v in vs],
        scratch_shapes=[
            pltpu.VMEM((row_blocks, 2, block, width), bf16),
            pltpu.VMEM((it, 2 * block), bf16),
        ],
        name="region",
    )(block_mask, *pieces, *vs, *dvs)
    keep, send = outs[:2]
    parts = outs[2:]

    item_bits = item_bits[::-1]
    held = list(parts)
    for bit in item_bits:
        back = swap(held.pop(), "au", n_au, bit)
        sizes = [h.shape[0] for h in held]
        cuts = [sum(sizes[:i]) for i in range(len(sizes))]
        held = [h + back[c : c + n] for h, c, n in zip(held, cuts, sizes)]
    item_product = held[0][0]

    bits = bits_of(1, n_ia)[::-1]
    acc = keep + swap(send, "ia", n_ia, bits[0])
    for bit in bits[1:]:
        if bit == members:
            acc = acc.reshape((row_blocks, us, width))
        half = acc.shape[0] // 2
        acc = acc[:half] + swap(acc[half:], "ia", n_ia, bit)
    user_product = acc.reshape(us, width)
    return user_product, item_product


def solution(mesh):
    n_au, n_ia = mesh.shape["au"], mesh.shape["ia"]
    placed = (
        P(("au", "ia"), None),
        P(("ia", "au"), None),
        P(("au", "ia"), None),
        P(("ia", "au"), None),
        P("au", "ia"),
    )
    return jax.shard_map(
        functools.partial(on_device, n_au=n_au, n_ia=n_ia),
        mesh=mesh,
        in_specs=placed,
        out_specs=(P(("au", "ia"), None), P(("ia", "au"), None)),
        check_vma=False,
    )
```

```python
import functools
import math

import jax
import jax.numpy as jnp
from jax import lax
from jax.experimental import pallas as pl
from jax.experimental.pallas import tpu as pltpu
from jax.sharding import PartitionSpec as P

f32 = jnp.float32
bf16 = jnp.bfloat16
NN = (((1,), (0,)), ((), ()))
NT = (((1,), (1,)), ((), ()))
TN = (((0,), (0,)), ((), ()))
dot = functools.partial(lax.dot_general, preferred_element_type=f32)
TILE = 256


def swap(x, axis, size, bits):
    return lax.ppermute(x, axis, [(i, i ^ bits) for i in range(size)])


def bits_of(low, high):
    out = []
    bit = high // 2
    while bit >= low:
        out.append(bit)
        bit //= 2
    return out


def relative(bits):
    order = [0]
    for bit in bits:
        order = order + [r ^ bit for r in order]
    return order


def region_kernel(*refs, n_users, rows_of, cols_of, scale, add_user, add_item):
    mask = refs[0]
    users = refs[1 : 1 + n_users]
    at = 1 + n_users
    fac_i, tan_i = refs[at : at + 2]
    at += 2
    user_in = refs[at] if add_user else None
    at += add_user
    item_in = refs[at] if add_item else None
    at += add_item
    user_out, item_out, u_all, c_all = refs[at:]

    n_a, _, us, _ = users[0].shape
    n_pieces, it_dev, _ = fac_i.shape
    me_row = lax.axis_index("ia") // rows_of[0]
    me_col = lax.axis_index("au")
    for b, ref in enumerate(users):
        for k in range(n_a):
            for ft in range(2):
                u_all[ft, pl.ds((b * n_a + k) * us, us), :] = ref[k, ft]
    total_rows = n_users * n_a * us
    tile = min(TILE, total_rows)
    in_tile = tile // us
    block = cols_of[0]
    lane = lax.broadcasted_iota(jnp.int32, (1, tile), 1)
    sub = min(TILE, it_dev)
    for t in range(total_rows // tile):
        rows = pl.ds(t * tile, tile)
        fac = u_all[0, rows, :]
        tan = u_all[1, rows, :]
        total = None
        for k in range(n_pieces):
            for ib in range(it_dev // sub):
                items = pl.ds(ib * sub, sub)
                v = fac_i[k, items, :]
                dv = tan_i[k, items, :]
                s = dot(v, fac, NT)
                tt = dot(v, tan, NT) + dot(dv, fac, NT)
                seen = []
                for i in range(sub // block):
                    col = (me_col ^ cols_of[1][k]) * (it_dev // block) + ib * (sub // block) + i
                    row = None
                    for j in reversed(range(in_tile)):
                        m = mask[me_row ^ rows_of[1][t * in_tile + j], col].astype(f32) * scale
                        full = jnp.full((1, tile), m, f32)
                        row = full if row is None else jnp.where(lane < (j + 1) * us, full, row)
                    seen.append(jnp.broadcast_to(row, (block, tile)))
                seen = jnp.concatenate(seen, 0)
                e = jnp.exp(jnp.abs(s) * -scale)
                p = 1.0 / (1.0 + e)
                c = (e * p * p * (tt * seen)).astype(bf16)
                c_all[items, :] = c
                r = dot(c, fac, NN) * scale
                if t > 0:
                    r = r + item_out[k, items, :]
                elif item_in is not None:
                    r = r + item_in[k, items, :]
                item_out[k, items, :] = r
            part = dot(c_all[...], fac_i[k], TN)
            total = part if total is None else total + part
        total = total * scale
        for j in range(in_tile):
            b, k = divmod(t * in_tile + j, n_a)
            r = total[j * us : (j + 1) * us]
            if user_in is not None:
                r = r + user_in[b, k]
            user_out[b, k] = r


def in_vmem(x):
    return pltpu.with_memory_space_constraint(x, pltpu.VMEM)


def region(mask, users, items, user_sum, item_sum, **static):
    vm = pl.BlockSpec(memory_space=pltpu.VMEM)
    n_a, _, us, width = users[0].shape
    n_pieces, it_dev, _ = items[0].shape
    given = [in_vmem(x) for x in (*users, *items)]
    aliases = {}
    if user_sum is not None:
        aliases[1 + len(given)] = 0
        given.append(in_vmem(user_sum))
    if item_sum is not None:
        aliases[1 + len(given)] = 1
        given.append(in_vmem(item_sum))
    total_rows = len(users) * n_a * us
    return pl.pallas_call(
        functools.partial(
            region_kernel,
            n_users=len(users),
            add_user=user_sum is not None,
            add_item=item_sum is not None,
            **static,
        ),
        in_specs=[pl.BlockSpec(memory_space=pltpu.SMEM)] + [vm] * len(given),
        out_specs=[vm, vm],
        out_shape=[
            pltpu.VMEM((len(users), n_a, us, width), f32),
            pltpu.VMEM((n_pieces, it_dev, width), f32),
        ],
        input_output_aliases=aliases,
        scratch_shapes=[
            pltpu.VMEM((2, total_rows, width), bf16),
            pltpu.VMEM((it_dev, min(TILE, total_rows)), bf16),
        ],
        compiler_params=pltpu.CompilerParams(vmem_limit_bytes=16 * 2**20),
    )(mask, *given)


def on_device(user_factors, item_factors, user_tangent, item_tangent, block_mask, n_au, n_ia):
    us, width = user_factors.shape
    row_blocks, _ = block_mask.shape
    block = us * n_ia // row_blocks
    members = block // us
    scale = 1.0 / math.sqrt(width)
    core, near = 1, [2, 4, 6]
    a_bits = bits_of(8, n_ia)

    item_bits = bits_of(1, n_au)
    facs, tans = [item_factors[None]], [item_tangent[None]]
    for n, bit in enumerate(item_bits):
        held_f = facs[0] if n == 0 else jnp.concatenate(facs, 0)
        held_t = tans[0] if n == 0 else jnp.concatenate(tans, 0)
        facs.append(swap(held_f, "au", n_au, bit))
        tans.append(swap(held_t, "au", n_au, bit))
    rel_items = relative(item_bits)

    far = jnp.stack([user_factors, user_tangent])[None]
    for n, bit in enumerate(a_bits):
        far = jnp.concatenate([far, swap(far, "ia", n_ia, bit)], 0)
    rel_a = relative(a_bits)
    mine = [far] + [swap(far, "ia", n_ia, b) for b in near]
    other = [swap(x, "ia", n_ia, core) for x in mine]
    rows_of = (members, [(b ^ r) // members for b in [0, *near] for r in rel_a])

    sums = {0: None, 1: None}
    item_sums = []
    at = 0
    for g, (f, t) in enumerate(zip(facs, tans)):
        n = f.shape[0]
        cols_of = (block, rel_items[at : at + n])
        at += n
        item_sum = None
        last = g == len(facs) - 1
        for half in (1, 0) if last else (0, 1):
            sums[half], item_sum = region(
                block_mask,
                other if half else mine,
                (f, t),
                sums[half],
                item_sum,
                rows_of=rows_of,
                cols_of=cols_of,
                scale=scale,
            )
        item_sums.append(item_sum)

    core_in = swap(sums[1], "ia", n_ia, core)
    for n, bit in enumerate(item_bits[::-1]):
        back = swap(item_sums.pop(), "au", n_au, bit)
        sizes = [h.shape[0] for h in item_sums]
        cuts = [sum(sizes[:i]) for i in range(len(sizes))]
        item_sums = [h + back[c : c + s] for h, c, s in zip(item_sums, cuts, sizes)]
    item_product = item_sums[0][0]

    keep = sums[0] + core_in
    acc = keep[0]
    for i, b in enumerate(near):
        acc = acc + swap(keep[i + 1], "ia", n_ia, b)
    for n, bit in enumerate(a_bits[::-1]):
        half = acc.shape[0] // 2
        acc = acc[:half] + swap(acc[half:], "ia", n_ia, bit)
    user_product = acc.reshape(us, width)
    return user_product, item_product


def solution(mesh):
    n_au, n_ia = mesh.shape["au"], mesh.shape["ia"]
    placed = (
        P(("au", "ia"), None),
        P(("ia", "au"), None),
        P(("au", "ia"), None),
        P(("ia", "au"), None),
        P("au", "ia"),
    )

    def body(*args):
        return on_device(*args, n_au=n_au, n_ia=n_ia)

    return jax.shard_map(
        body,
        mesh=mesh,
        in_specs=placed,
        out_specs=(P(("au", "ia"), None), P(("ia", "au"), None)),
        check_vma=False,
    )
```

```python
import functools
import math

import jax
import jax.numpy as jnp
from jax import lax
from jax.experimental import pallas as pl
from jax.experimental.pallas import tpu as pltpu
from jax.sharding import PartitionSpec as P

f32 = jnp.float32
bf16 = jnp.bfloat16
NN = (((1,), (0,)), ((), ()))
NT = (((1,), (1,)), ((), ()))
TN = (((0,), (0,)), ((), ()))
dot = functools.partial(lax.dot_general, preferred_element_type=f32)
TILE = 256


def swap(x, axis, size, bits):
    return lax.ppermute(x, axis, [(i, i ^ bits) for i in range(size)])


def bits_of(low, high):
    out = []
    bit = high // 2
    while bit >= low:
        out.append(bit)
        bit //= 2
    return out


def relative(bits):
    order = [0]
    for bit in bits:
        order = order + [r ^ bit for r in order]
    return order


def region_kernel(*refs, n_users, rows_of, cols_of, scale, add_user, add_item):
    mask = refs[0]
    users = refs[1 : 1 + n_users]
    at = 1 + n_users
    fac_i, tan_i = refs[at : at + 2]
    at += 2
    user_in = refs[at : at + n_users] if add_user else None
    at += n_users * add_user
    item_in = refs[at] if add_item else None
    at += add_item
    user_out = refs[at : at + n_users]
    item_out, u_all, c_all = refs[at + n_users :]

    n_a, _, us, _ = users[0].shape
    n_pieces, it_dev, _ = fac_i.shape
    me_row = lax.axis_index("ia") // rows_of[0]
    me_col = lax.axis_index("au")
    for b, ref in enumerate(users):
        for k in range(n_a):
            for ft in range(2):
                u_all[ft, pl.ds((b * n_a + k) * us, us), :] = ref[k, ft]
    total_rows = n_users * n_a * us
    tile = min(TILE, total_rows)
    in_tile = tile // us
    block = cols_of[0]
    lane = lax.broadcasted_iota(jnp.int32, (1, tile), 1)
    sub = min(TILE, it_dev)
    for t in range(total_rows // tile):
        rows = pl.ds(t * tile, tile)
        fac = u_all[0, rows, :]
        tan = u_all[1, rows, :]
        total = None
        for k in range(n_pieces):
            for ib in range(it_dev // sub):
                items = pl.ds(ib * sub, sub)
                v = fac_i[k, items, :]
                dv = tan_i[k, items, :]
                if 2 * tile <= TILE:
                    both = dot(v, jnp.concatenate([fac, tan], 0), NT)
                    s = both[:, :tile]
                    tt = both[:, tile:] + dot(dv, fac, NT)
                else:
                    s = dot(v, fac, NT)
                    tt = dot(v, tan, NT) + dot(dv, fac, NT)
                seen = []
                for i in range(sub // block):
                    col = (me_col ^ cols_of[1][k]) * (it_dev // block) + ib * (sub // block) + i
                    row = None
                    for j in reversed(range(in_tile)):
                        m = mask[me_row ^ rows_of[1][t * in_tile + j], col].astype(f32) * scale
                        full = jnp.full((1, tile), m, f32)
                        row = full if row is None else jnp.where(lane < (j + 1) * us, full, row)
                    seen.append(jnp.broadcast_to(row, (block, tile)))
                seen = jnp.concatenate(seen, 0)
                e = jnp.exp(jnp.abs(s) * -scale)
                p = 1.0 / (1.0 + e)
                c = (e * p * p * (tt * seen)).astype(bf16)
                c_all[items, :] = c
                r = dot(c, fac, NN) * scale
                if t > 0:
                    r = r + item_out[k, items, :]
                elif item_in is not None:
                    r = r + item_in[k, items, :]
                item_out[k, items, :] = r
            part = dot(c_all[...], fac_i[k], TN)
            total = part if total is None else total + part
        total = total * scale
        for j in range(in_tile):
            b, k = divmod(t * in_tile + j, n_a)
            r = total[j * us : (j + 1) * us]
            if user_in is not None:
                r = r + user_in[b][k]
            user_out[b][k] = r


def in_vmem(x):
    return pltpu.with_memory_space_constraint(x, pltpu.VMEM)


VM = pl.BlockSpec(memory_space=pltpu.VMEM)
PARAMS = pltpu.CompilerParams(vmem_limit_bytes=16 * 2**20)


def region(mask, users, items, user_sums, item_sum, **static):
    n_a, _, us, width = users[0].shape
    n_pieces, it_dev, _ = items[0].shape
    given = [in_vmem(x) for x in (*users, *items)]
    aliases = {}
    add_user = user_sums[0] is not None
    if add_user:
        for n, x in enumerate(user_sums):
            aliases[1 + len(given)] = n
            given.append(in_vmem(x))
    if item_sum is not None:
        aliases[1 + len(given)] = len(users)
        given.append(in_vmem(item_sum))
    total_rows = len(users) * n_a * us
    *user_sums, item_sum = pl.pallas_call(
        functools.partial(
            region_kernel, n_users=len(users), add_user=add_user, add_item=item_sum is not None, **static
        ),
        in_specs=[pl.BlockSpec(memory_space=pltpu.SMEM)] + [VM] * len(given),
        out_specs=[VM] * (len(users) + 1),
        out_shape=[pltpu.VMEM((n_a, us, width), f32)] * len(users)
        + [pltpu.VMEM((n_pieces, it_dev, width), f32)],
        input_output_aliases=aliases,
        scratch_shapes=[pltpu.VMEM((2, total_rows, width), bf16), pltpu.VMEM((it_dev, min(TILE, total_rows)), bf16)],
        compiler_params=PARAMS,
    )(mask, *given)
    return user_sums, item_sum


def load_kernel(*refs):
    n = (len(refs) - 1) // 2
    sems = refs[-1]
    copies = [pltpu.make_async_copy(refs[i], refs[n + i], sems.at[i]) for i in range(n)]
    for c in copies:
        c.start()
    for c in copies:
        c.wait()


def load(arrays):
    return pl.pallas_call(
        load_kernel,
        in_specs=[pl.BlockSpec(memory_space=pl.ANY)] * len(arrays),
        out_specs=[VM] * len(arrays),
        out_shape=[pltpu.VMEM(x.shape, x.dtype) for x in arrays],
        scratch_shapes=[pltpu.SemaphoreType.DMA((len(arrays),))],
        compiler_params=PARAMS,
    )(*[pltpu.with_memory_space_constraint(x, pltpu.HBM) for x in arrays])


GROUPS = 16


def encode_kernel(x_ref, out_ref):
    n, rows, _ = x_ref.shape
    step = rows // GROUPS
    for k in range(n):
        exps = []
        for g in range(GROUPS):
            x = x_ref[k, pl.ds(g * step, step), :]
            top = jnp.max(jnp.abs(x), 0, keepdims=True)
            e = 14.0 - jnp.ceil(jnp.log2(jnp.maximum(top, 1e-30)))
            out_ref[k, pl.ds(g * step, step), :] = jnp.round(x * jnp.exp2(e)).astype(jnp.int32).astype(jnp.int16)
            exps.append(e)
        out_ref[k, pl.ds(rows, GROUPS), :] = jnp.concatenate(exps, 0).astype(jnp.int32).astype(jnp.int16)


def encode(x):
    n, rows, width = x.shape
    return pl.pallas_call(
        encode_kernel,
        in_specs=[VM],
        out_specs=VM,
        out_shape=pltpu.VMEM((n, rows + GROUPS, width), jnp.int16),
        compiler_params=PARAMS,
    )(in_vmem(x))


def decode_kernel(x_ref, q_ref, out_ref, *, at):
    n, rows, _ = x_ref.shape
    step = rows // GROUPS
    for k in range(n):
        unit = jnp.exp2(-q_ref[at + k, pl.ds(rows, GROUPS), :].astype(jnp.int32).astype(f32))
        for g in range(GROUPS):
            part = pl.ds(g * step, step)
            out_ref[k, part, :] = x_ref[k, part, :] + q_ref[at + k, part, :].astype(jnp.int32).astype(f32) * unit[g : g + 1]


def add_decoded(x, q, at):
    return pl.pallas_call(
        functools.partial(decode_kernel, at=at),
        in_specs=[VM, VM],
        out_specs=VM,
        out_shape=jax.ShapeDtypeStruct(x.shape, f32),
        compiler_params=PARAMS,
    )(in_vmem(x), in_vmem(q))


def on_device(user_factors, item_factors, user_tangent, item_tangent, block_mask, n_au, n_ia):
    us, width = user_factors.shape
    row_blocks, _ = block_mask.shape
    block = us * n_ia // row_blocks
    members = block // us
    assert members == 4
    scale = 1.0 / math.sqrt(width)
    core, near = 1, 2
    a_bits = bits_of(members, n_ia)
    rel_a = relative(a_bits)
    row_of = [r // members for r in rel_a]

    far = jnp.stack([user_factors, user_tangent])[None]
    for n, bit in enumerate(a_bits):
        far = jnp.concatenate([far, swap(far, "ia", n_ia, bit)], 0)

    item_bits = bits_of(1, n_au)
    rel_items = relative(item_bits)
    facs, tans = [item_factors[None]], [item_tangent[None]]
    for n, bit in enumerate(item_bits):
        held_f = facs[0] if n == 0 else jnp.concatenate(facs, 0)
        held_t = tans[0] if n == 0 else jnp.concatenate(tans, 0)
        facs.append(swap(held_f, "au", n_au, bit))
        tans.append(swap(held_t, "au", n_au, bit))
    facs[0], tans[0] = load((facs[0], tans[0]))

    pieces = [far, swap(far, "ia", n_ia, core), swap(far, "ia", n_ia, near)]
    pieces.append(swap(pieces[2], "ia", n_ia, core))
    user_sums = [None] * 4
    item_sums = []
    at = 0
    for g, (f, t) in enumerate(zip(facs, tans)):
        n = f.shape[0]
        cols_of = (block, rel_items[at : at + n])
        at += n
        item_sum = None
        for which in [(0, 1), (2,), (3,)] if g == 0 else [(1, 3), (0, 2)]:
            sums, item_sum = region(
                block_mask,
                [pieces[w] for w in which],
                (f, t),
                [user_sums[w] for w in which],
                item_sum,
                rows_of=(members, row_of * len(which)),
                cols_of=cols_of,
                scale=scale,
            )
            for w, x in zip(which, sums):
                user_sums[w] = x
        item_sums.append(item_sum)

    sent = [swap(user_sums[w], "ia", n_ia, core) for w in (1, 3)]
    for n, bit in enumerate(item_bits[::-1]):
        back = swap(encode(item_sums.pop()), "au", n_au, bit)
        sizes = [h.shape[0] for h in item_sums]
        cuts = [sum(sizes[:i]) for i in range(len(sizes))]
        item_sums = [add_decoded(h, back, c) for h, c in zip(item_sums, cuts)]
    item_product = item_sums[0][0]

    keep = [user_sums[0] + sent[0], user_sums[2] + sent[1]]
    half = len(rel_a) // 2
    last = a_bits[-1]
    acc = keep[0][:half]
    acc = acc + swap(keep[1][:half], "ia", n_ia, near)
    acc = acc + swap(keep[0][half:], "ia", n_ia, last)
    acc = acc + swap(keep[1][half:], "ia", n_ia, near ^ last)
    for n, bit in enumerate(a_bits[:-1][::-1]):
        half = acc.shape[0] // 2
        acc = acc[:half] + swap(acc[half:], "ia", n_ia, bit)
    user_product = acc.reshape(us, width)
    return user_product, item_product


def solution(mesh):
    n_au, n_ia = mesh.shape["au"], mesh.shape["ia"]
    placed = (
        P(("au", "ia"), None),
        P(("ia", "au"), None),
        P(("au", "ia"), None),
        P(("ia", "au"), None),
        P("au", "ia"),
    )

    def body(*args):
        return on_device(*args, n_au=n_au, n_ia=n_ia)

    return jax.shard_map(
        body,
        mesh=mesh,
        in_specs=placed,
        out_specs=(P(("au", "ia"), None), P(("ia", "au"), None)),
        check_vma=False,
    )
```

```python
import functools
import math

import jax
import jax.numpy as jnp
from jax import lax
from jax.experimental import pallas as pl
from jax.experimental.pallas import tpu as pltpu
from jax.sharding import PartitionSpec as P

f32 = jnp.float32
bf16 = jnp.bfloat16
NN = (((1,), (0,)), ((), ()))
NT = (((1,), (1,)), ((), ()))
TN = (((0,), (0,)), ((), ()))
dot = functools.partial(lax.dot_general, preferred_element_type=f32)
TILE = 256


def swap(x, axis, size, bits):
    return lax.ppermute(x, axis, [(i, i ^ bits) for i in range(size)])


def bits_of(low, high):
    out = []
    bit = high // 2
    while bit >= low:
        out.append(bit)
        bit //= 2
    return out


def relative(bits):
    order = [0]
    for bit in bits:
        order = order + [r ^ bit for r in order]
    return order


def region_kernel(*refs, n_users, sums_at, n_sums, add_item, lanes, cols, scale):
    seen_ref = refs[0]
    users = refs[1 : 1 + n_users]
    at = 1 + n_users
    fac_i, tan_i = refs[at : at + 2]
    at += 2
    user_in = refs[at : at + n_sums]
    at += n_sums
    item_in = refs[at] if add_item else None
    at += add_item
    user_out, item_out, u_all, c_all = refs[at:]

    n_a, _, us, _ = users[0].shape
    n_pieces, it_dev, _ = fac_i.shape
    for b, ref in enumerate(users):
        for k in range(n_a):
            for ft in range(2):
                u_all[ft, pl.ds((b * n_a + k) * us, us), :] = ref[k, ft]
    total_rows = n_users * n_a * us
    tile = min(TILE, total_rows)
    in_tile = tile // us
    blocks = cols[1]
    block = it_dev // blocks
    sub = min(TILE, it_dev)
    for t in range(total_rows // tile):
        rows = pl.ds(t * tile, tile)
        fac = u_all[0, rows, :]
        tan = u_all[1, rows, :]
        total = None
        for k in range(n_pieces):
            for ib in range(it_dev // sub):
                items = pl.ds(ib * sub, sub)
                v = fac_i[k, items, :]
                dv = tan_i[k, items, :]
                if 2 * tile <= TILE:
                    both = dot(v, jnp.concatenate([fac, tan], 0), NT)
                    s = both[:, :tile]
                    tt = both[:, tile:] + dot(dv, fac, NT)
                else:
                    s = dot(v, fac, NT)
                    tt = dot(v, tan, NT) + dot(dv, fac, NT)
                seen = []
                for i in range(sub // block):
                    row = seen_ref[
                        pl.ds((cols[0] + k) * blocks + ib * (sub // block) + i, 1), pl.ds(lanes + t * tile, tile)
                    ]
                    seen.append(jnp.broadcast_to(row, (block, tile)))
                seen = jnp.concatenate(seen, 0)
                e = jnp.exp(jnp.abs(s) * -scale)
                p = 1.0 / (1.0 + e)
                c = (e * p * p * (tt * seen)).astype(bf16)
                c_all[k, items, pl.ds(0, tile)] = c
            r = dot(c_all[k], fac, NN) * scale
            if t > 0:
                r = r + item_out[k]
            elif item_in is not None:
                r = r + item_in[k]
            item_out[k] = r
            part = dot(c_all[k], fac_i[k], TN)
            total = part if total is None else total + part
        total = total * scale
        for j in range(in_tile):
            b, k = divmod(t * in_tile + j, n_a)
            r = total[j * us : (j + 1) * us]
            if n_sums:
                r = r + user_in[sums_at[b][0]][sums_at[b][1], k]
            user_out[b, k] = r


def in_vmem(x):
    return pltpu.with_memory_space_constraint(x, pltpu.VMEM)


VM = pl.BlockSpec(memory_space=pltpu.VMEM)
PARAMS = pltpu.CompilerParams(vmem_limit_bytes=16 * 2**20)


def region(seen, users, items, sums, sums_at, item_sum, **static):
    n_a, _, us, width = users[0].shape
    n_pieces, it_dev, _ = items[0].shape
    given = [in_vmem(x) for x in (seen, *users, *items, *sums)]
    aliases = {}
    if item_sum is not None:
        aliases[len(given)] = 1
        given.append(in_vmem(item_sum))
    total_rows = len(users) * n_a * us
    return pl.pallas_call(
        functools.partial(
            region_kernel,
            n_users=len(users),
            sums_at=sums_at,
            n_sums=len(sums),
            add_item=item_sum is not None,
            **static,
        ),
        in_specs=[VM] * len(given),
        out_specs=[VM] * 2,
        out_shape=[
            pltpu.VMEM((len(users), n_a, us, width), f32),
            pltpu.VMEM((n_pieces, it_dev, width), f32),
        ],
        input_output_aliases=aliases,
        scratch_shapes=[
            pltpu.VMEM((2, total_rows, width), bf16),
            pltpu.VMEM((n_pieces, it_dev, min(TILE, total_rows)), bf16),
        ],
        compiler_params=PARAMS,
    )(*given)


def load_kernel(mask, fac, tan, fac_out, tan_out, seen, sems, *, rows_of, cols_of, us, scale):
    copies = [
        pltpu.make_async_copy(fac, fac_out, sems.at[0]),
        pltpu.make_async_copy(tan, tan_out, sems.at[1]),
    ]
    for c in copies:
        c.start()
    per, order = cols_of
    members, rows = rows_of
    me_row = lax.axis_index("ia") // members
    me_col = lax.axis_index("au")
    lane = lax.broadcasted_iota(jnp.int32, (1, seen.shape[1]), 1)
    for q, rel in enumerate(order):
        for i in range(per):
            value = {r: mask[me_row ^ r, (me_col ^ rel) * per + i].astype(f32) * scale for r in sorted(set(rows))}
            line = None
            for j in reversed(range(len(rows))):
                full = jnp.full(lane.shape, value[rows[j]], f32)
                line = full if line is None else jnp.where(lane < (j + 1) * us, full, line)
            seen[pl.ds(q * per + i, 1), :] = line
    for c in copies:
        c.wait()


def load(mask, fac, tan, **static):
    hbm = [pltpu.with_memory_space_constraint(x, pltpu.HBM) for x in (fac, tan)]
    blocks = static["cols_of"][0] * len(static["cols_of"][1])
    lanes = len(static["rows_of"][1]) * static["us"]
    return pl.pallas_call(
        functools.partial(load_kernel, **static),
        in_specs=[pl.BlockSpec(memory_space=pltpu.SMEM)] + [pl.BlockSpec(memory_space=pltpu.HBM)] * 2,
        out_specs=[VM] * 3,
        out_shape=[pltpu.VMEM(fac.shape, fac.dtype), pltpu.VMEM(tan.shape, tan.dtype), pltpu.VMEM((blocks, lanes), f32)],
        scratch_shapes=[pltpu.SemaphoreType.DMA((2,))],
        compiler_params=PARAMS,
    )(mask, *hbm)


def stack_kernel(a, b, out, sems):
    copies = [
        pltpu.make_async_copy(a, out.at[0, 0], sems.at[0]),
        pltpu.make_async_copy(b, out.at[0, 1], sems.at[1]),
    ]
    for c in copies:
        c.start()
    for c in copies:
        c.wait()


def stack(a, b):
    return pl.pallas_call(
        stack_kernel,
        in_specs=[pl.BlockSpec(memory_space=pltpu.HBM)] * 2,
        out_specs=VM,
        out_shape=pltpu.VMEM((1, 2, *a.shape), a.dtype),
        scratch_shapes=[pltpu.SemaphoreType.DMA((2,))],
        compiler_params=PARAMS,
    )(*[pltpu.with_memory_space_constraint(x, pltpu.HBM) for x in (a, b)])


GROUPS = 16


def encode_kernel(x_ref, out_ref):
    n, rows, _ = x_ref.shape
    step = rows // GROUPS
    for k in range(n):
        exps = []
        for g in range(GROUPS):
            x = x_ref[k, pl.ds(g * step, step), :]
            top = jnp.max(jnp.abs(x), 0, keepdims=True)
            e = 14.0 - jnp.ceil(jnp.log2(jnp.maximum(top, 1e-30)))
            out_ref[k, pl.ds(g * step, step), :] = jnp.round(x * jnp.exp2(e)).astype(jnp.int32).astype(jnp.int16)
            exps.append(e)
        out_ref[k, pl.ds(rows, GROUPS), :] = jnp.concatenate(exps, 0).astype(jnp.int32).astype(jnp.int16)


def encode(x):
    n, rows, width = x.shape
    return pl.pallas_call(
        encode_kernel,
        in_specs=[VM],
        out_specs=VM,
        out_shape=pltpu.VMEM((n, rows + GROUPS, width), jnp.int16),
        compiler_params=PARAMS,
    )(in_vmem(x))


def decode_kernel(x_ref, q_ref, out_ref, *, at):
    n, rows, _ = x_ref.shape
    step = rows // GROUPS
    for k in range(n):
        unit = jnp.exp2(-q_ref[at + k, pl.ds(rows, GROUPS), :].astype(jnp.int32).astype(f32))
        for g in range(GROUPS):
            part = pl.ds(g * step, step)
            out_ref[k, part, :] = x_ref[k, part, :] + q_ref[at + k, part, :].astype(jnp.int32).astype(f32) * unit[g : g + 1]


def add_decoded(x, q, at):
    return pl.pallas_call(
        functools.partial(decode_kernel, at=at),
        in_specs=[VM, VM],
        out_specs=VM,
        out_shape=jax.ShapeDtypeStruct(x.shape, f32),
        compiler_params=PARAMS,
    )(in_vmem(x), in_vmem(q))


def on_device(user_factors, item_factors, user_tangent, item_tangent, block_mask, n_au, n_ia):
    us, width = user_factors.shape
    row_blocks, per = block_mask.shape
    per //= n_au
    members = us * n_ia // row_blocks // us
    assert members == 4
    scale = 1.0 / math.sqrt(width)
    core, near = 1, [0, 2, 4, 6]
    a_bits = bits_of(8, n_ia)
    rel_a = relative(a_bits)

    far = stack(user_factors, user_tangent)
    for bit in a_bits:
        far = jnp.concatenate([far, swap(far, "ia", n_ia, bit)], 0)

    item_bits = bits_of(1, n_au)
    rel_items = relative(item_bits)
    facs, tans = [item_factors[None]], [item_tangent[None]]
    for n, bit in enumerate(item_bits):
        held_f = facs[0] if n == 0 else jnp.concatenate(facs, 0)
        held_t = tans[0] if n == 0 else jnp.concatenate(tans, 0)
        facs.append(swap(held_f, "au", n_au, bit))
        tans.append(swap(held_t, "au", n_au, bit))
    rows = [(b ^ r) // members for b in near for r in rel_a]
    facs[0], tans[0], seen = load(
        block_mask, facs[0], tans[0], rows_of=(members, rows), cols_of=(per, rel_items), us=us, scale=scale
    )
    piece = len(rel_a) * us

    mine = [far] + [swap(far, "ia", n_ia, b) for b in near[1:]]
    other = [swap(x, "ia", n_ia, core) for x in mine]

    def call(users, g, sums, sums_at, item_sum, lanes=0):
        at = sum(f.shape[0] for f in facs[:g])
        return region(
            seen, users, (facs[g], tans[g]), sums, sums_at, item_sum, lanes=lanes, cols=(at, per), scale=scale
        )

    first, item_sum = call([mine[0], other[0]], 0, [], None, None)
    second, item_sum = call([mine[1], other[1], mine[2], other[2]], 0, [], None, item_sum)
    third, own_items = call([mine[3], other[3]], 0, [], None, item_sum, lanes=2 * piece)
    sums = [first, second, third]
    at_mine, at_other = [(0, 0), (1, 0), (1, 2), (2, 0)], [(0, 1), (1, 1), (1, 3), (2, 1)]
    item_sums = [own_items]
    for g in range(1, len(facs)):
        out_other, item_sum = call(other, g, sums, at_other, None)
        out_mine, item_sum = call(mine, g, sums, at_mine, item_sum)
        item_sums.append(item_sum)
        sums = [out_mine, out_other]
        at_mine, at_other = [(0, i) for i in range(4)], [(1, i) for i in range(4)]

    keep = out_mine + swap(out_other, "ia", n_ia, core)
    acc = keep[0]
    for n, b in enumerate(near[1:]):
        acc = acc + swap(keep[n + 1], "ia", n_ia, b)
    for bit in a_bits[::-1]:
        half = acc.shape[0] // 2
        acc = acc[:half] + swap(acc[half:], "ia", n_ia, bit)
    user_product = acc.reshape(us, width)

    for bit in item_bits[::-1]:
        back = swap(encode(item_sums.pop()), "au", n_au, bit)
        sizes = [h.shape[0] for h in item_sums]
        cuts = [sum(sizes[:i]) for i in range(len(sizes))]
        item_sums = [add_decoded(h, back, c) for h, c in zip(item_sums, cuts)]
    item_product = item_sums[0][0]
    return user_product, item_product


def solution(mesh):
    n_au, n_ia = mesh.shape["au"], mesh.shape["ia"]
    placed = (
        P(("au", "ia"), None),
        P(("ia", "au"), None),
        P(("au", "ia"), None),
        P(("ia", "au"), None),
        P("au", "ia"),
    )

    def body(*args):
        return on_device(*args, n_au=n_au, n_ia=n_ia)

    return jax.shard_map(
        body,
        mesh=mesh,
        in_specs=placed,
        out_specs=(P(("au", "ia"), None), P(("ia", "au"), None)),
        check_vma=False,
    )
```

```python
import functools
import math

import jax
import jax.numpy as jnp
from jax import lax
from jax.experimental import pallas as pl
from jax.experimental.pallas import tpu as pltpu
from jax.sharding import PartitionSpec as P

f32 = jnp.float32
bf16 = jnp.bfloat16
NN = (((1,), (0,)), ((), ()))
NT = (((1,), (1,)), ((), ()))
TN = (((0,), (0,)), ((), ()))
dot = functools.partial(lax.dot_general, preferred_element_type=f32)
TILE = 256


def swap(x, axis, size, bits):
    return lax.ppermute(x, axis, [(i, i ^ bits) for i in range(size)])


def bits_of(low, high):
    out = []
    bit = high // 2
    while bit >= low:
        out.append(bit)
        bit //= 2
    return out


def relative(bits):
    order = [0]
    for bit in bits:
        order = order + [r ^ bit for r in order]
    return order


def region_kernel(*refs, n_users, sums_at, n_sums, add_item, lanes, cols, scale):
    seen_ref = refs[0]
    users = refs[1 : 1 + n_users]
    at = 1 + n_users
    fac_i, tan_i = refs[at : at + 2]
    at += 2
    user_in = refs[at : at + n_sums]
    at += n_sums
    item_in = refs[at] if add_item else None
    at += add_item
    user_out, item_out, u_all, c_all = refs[at:]

    n_a, _, us, _ = users[0].shape
    n_pieces, it_dev, _ = fac_i.shape
    for b, ref in enumerate(users):
        for k in range(n_a):
            for ft in range(2):
                u_all[ft, pl.ds((b * n_a + k) * us, us), :] = ref[k, ft]
    total_rows = n_users * n_a * us
    tile = min(TILE, total_rows)
    in_tile = tile // us
    blocks = cols[1]
    block = it_dev // blocks
    sub = min(TILE, it_dev)
    for t in range(total_rows // tile):
        rows = pl.ds(t * tile, tile)
        fac = u_all[0, rows, :]
        tan = u_all[1, rows, :]
        total = None
        for k in range(n_pieces):
            for ib in range(it_dev // sub):
                items = pl.ds(ib * sub, sub)
                v = fac_i[k, items, :]
                dv = tan_i[k, items, :]
                if 2 * tile <= TILE:
                    both = dot(v, jnp.concatenate([fac, tan], 0), NT)
                    s = both[:, :tile]
                    tt = both[:, tile:] + dot(dv, fac, NT)
                else:
                    s = dot(v, fac, NT)
                    tt = dot(v, tan, NT) + dot(dv, fac, NT)
                seen = []
                for i in range(sub // block):
                    row = seen_ref[
                        pl.ds((cols[0] + k) * blocks + ib * (sub // block) + i, 1), pl.ds(lanes + t * tile, tile)
                    ]
                    seen.append(jnp.broadcast_to(row, (block, tile)))
                seen = jnp.concatenate(seen, 0)
                e = jnp.exp(jnp.abs(s) * -scale)
                p = 1.0 / (1.0 + e)
                c = (e * p * p * (tt * seen)).astype(bf16)
                c_all[k, items, pl.ds(0, tile)] = c
            r = dot(c_all[k], fac, NN) * scale
            if t > 0:
                r = r + item_out[k]
            elif item_in is not None:
                r = r + item_in[k]
            item_out[k] = r
            part = dot(c_all[k], fac_i[k], TN)
            total = part if total is None else total + part
        total = total * scale
        for j in range(in_tile):
            b, k = divmod(t * in_tile + j, n_a)
            r = total[j * us : (j + 1) * us]
            if n_sums:
                r = r + user_in[sums_at[b][0]][sums_at[b][1], k]
            user_out[b, k] = r


def in_vmem(x):
    return pltpu.with_memory_space_constraint(x, pltpu.VMEM)


VM = pl.BlockSpec(memory_space=pltpu.VMEM)
PARAMS = pltpu.CompilerParams(vmem_limit_bytes=16 * 2**20)


def region(seen, users, items, sums, sums_at, item_sum, **static):
    n_a, _, us, width = users[0].shape
    n_pieces, it_dev, _ = items[0].shape
    given = [in_vmem(x) for x in (seen, *users, *items, *sums)]
    aliases = {}
    if item_sum is not None:
        aliases[len(given)] = 1
        given.append(in_vmem(item_sum))
    total_rows = len(users) * n_a * us
    return pl.pallas_call(
        functools.partial(
            region_kernel,
            n_users=len(users),
            sums_at=sums_at,
            n_sums=len(sums),
            add_item=item_sum is not None,
            **static,
        ),
        in_specs=[VM] * len(given),
        out_specs=[VM] * 2,
        out_shape=[
            pltpu.VMEM((len(users), n_a, us, width), f32),
            pltpu.VMEM((n_pieces, it_dev, width), f32),
        ],
        input_output_aliases=aliases,
        scratch_shapes=[
            pltpu.VMEM((2, total_rows, width), bf16),
            pltpu.VMEM((n_pieces, it_dev, min(TILE, total_rows)), bf16),
        ],
        compiler_params=PARAMS,
    )(*given)


def load_kernel(mask, fac, tan, fac_out, tan_out, seen, sems, *, rows_of, cols_of, us, scale):
    copies = [
        pltpu.make_async_copy(fac, fac_out, sems.at[0]),
        pltpu.make_async_copy(tan, tan_out, sems.at[1]),
    ]
    for c in copies:
        c.start()
    per, order = cols_of
    members, rows = rows_of
    me_row = lax.axis_index("ia") // members
    me_col = lax.axis_index("au")
    lane = lax.broadcasted_iota(jnp.int32, (1, seen.shape[1]), 1)
    for q, rel in enumerate(order):
        for i in range(per):
            value = {r: mask[me_row ^ r, (me_col ^ rel) * per + i].astype(f32) * scale for r in sorted(set(rows))}
            line = None
            for j in reversed(range(len(rows))):
                full = jnp.full(lane.shape, value[rows[j]], f32)
                line = full if line is None else jnp.where(lane < (j + 1) * us, full, line)
            seen[pl.ds(q * per + i, 1), :] = line
    for c in copies:
        c.wait()


def load(mask, fac, tan, **static):
    hbm = [pltpu.with_memory_space_constraint(x, pltpu.HBM) for x in (fac, tan)]
    blocks = static["cols_of"][0] * len(static["cols_of"][1])
    lanes = len(static["rows_of"][1]) * static["us"]
    return pl.pallas_call(
        functools.partial(load_kernel, **static),
        in_specs=[pl.BlockSpec(memory_space=pltpu.SMEM)] + [pl.BlockSpec(memory_space=pltpu.HBM)] * 2,
        out_specs=[VM] * 3,
        out_shape=[pltpu.VMEM(fac.shape, fac.dtype), pltpu.VMEM(tan.shape, tan.dtype), pltpu.VMEM((blocks, lanes), f32)],
        scratch_shapes=[pltpu.SemaphoreType.DMA((2,))],
        compiler_params=PARAMS,
    )(mask, *hbm)


def stack_kernel(a, b, out, sems):
    copies = [
        pltpu.make_async_copy(a, out.at[0, 0], sems.at[0]),
        pltpu.make_async_copy(b, out.at[0, 1], sems.at[1]),
    ]
    for c in copies:
        c.start()
    for c in copies:
        c.wait()


def stack(a, b):
    return pl.pallas_call(
        stack_kernel,
        in_specs=[pl.BlockSpec(memory_space=pltpu.HBM)] * 2,
        out_specs=VM,
        out_shape=pltpu.VMEM((1, 2, *a.shape), a.dtype),
        scratch_shapes=[pltpu.SemaphoreType.DMA((2,))],
        compiler_params=PARAMS,
    )(*[pltpu.with_memory_space_constraint(x, pltpu.HBM) for x in (a, b)])


GROUPS = 16


def encode_rows(x, out_ref, k):
    rows = x.shape[0]
    groups = min(GROUPS, rows // GROUPS)
    step = rows // groups
    exps = []
    for g in range(groups):
        part = x[g * step : (g + 1) * step]
        top = jnp.max(jnp.abs(part), 0, keepdims=True)
        e = 14.0 - jnp.ceil(jnp.log2(jnp.maximum(top, 1e-30)))
        out_ref[k, pl.ds(g * step, step), :] = jnp.round(part * jnp.exp2(e)).astype(jnp.int32).astype(jnp.int16)
        exps.append(e)
    exps += exps[-1:] * (GROUPS - groups)
    out_ref[k, pl.ds(rows, GROUPS), :] = jnp.concatenate(exps, 0).astype(jnp.int32).astype(jnp.int16)


def decode_rows(q_ref, k, g, groups):
    rows = q_ref.shape[1] - GROUPS
    step = rows // groups
    unit = jnp.exp2(-q_ref[k, pl.ds(rows, GROUPS), :].astype(jnp.int32).astype(f32))
    return q_ref[k, pl.ds(g * step, step), :].astype(jnp.int32).astype(f32) * unit[g : g + 1]


def encode_kernel(x_ref, out_ref):
    for k in range(x_ref.shape[0]):
        encode_rows(x_ref[k], out_ref, k)


def encode(x):
    n, rows, width = x.shape
    return pl.pallas_call(
        encode_kernel,
        in_specs=[VM],
        out_specs=VM,
        out_shape=pltpu.VMEM((n, rows + GROUPS, width), jnp.int16),
        compiler_params=PARAMS,
    )(in_vmem(x))


def decode_kernel(x_ref, q_ref, out_ref, *, at):
    n, rows, _ = x_ref.shape
    groups = min(GROUPS, rows // GROUPS)
    step = rows // groups
    for k in range(n):
        for g in range(groups):
            part = pl.ds(g * step, step)
            out_ref[k, part, :] = x_ref[k, part, :] + decode_rows(q_ref, at + k, g, groups)


def add_decoded(x, q, at):
    return pl.pallas_call(
        functools.partial(decode_kernel, at=at),
        in_specs=[VM, VM],
        out_specs=VM,
        out_shape=jax.ShapeDtypeStruct(x.shape, f32),
        compiler_params=PARAMS,
    )(in_vmem(x), in_vmem(q))


def fold_kernel(mine, core_in, own, *coded):
    n, n_a, us, width = mine.shape
    own[0] = (mine[0] + core_in[0]).reshape(n_a * us, width)
    for i in range(1, n):
        encode_rows((mine[i] + core_in[i]).reshape(n_a * us, width), coded[i - 1], 0)


def fold(mine, core_in):
    n, n_a, us, width = mine.shape
    rows = n_a * us
    return pl.pallas_call(
        fold_kernel,
        in_specs=[VM, VM],
        out_specs=[VM] * n,
        out_shape=[pltpu.VMEM((1, rows, width), f32)]
        + [pltpu.VMEM((1, rows + GROUPS, width), jnp.int16)] * (n - 1),
        compiler_params=PARAMS,
    )(in_vmem(mine), in_vmem(core_in))


def near_kernel(own, *refs):
    *coded, keep, send = refs
    rows = own.shape[1]
    half = rows // 2
    groups = min(GROUPS, rows // GROUPS)
    step = rows // groups
    for g in range(groups):
        x = own[0, pl.ds(g * step, step), :]
        for q in coded:
            x = x + decode_rows(q, 0, g, groups)
        to, at = (keep, g * step) if g * step < half else (send, g * step - half)
        to[pl.ds(at, step), :] = x


def near_sum(own, coded):
    _, rows, width = own.shape
    return pl.pallas_call(
        near_kernel,
        in_specs=[VM] * (1 + len(coded)),
        out_specs=[VM] * 2,
        out_shape=[pltpu.VMEM((rows // 2, width), f32)] * 2,
        compiler_params=PARAMS,
    )(*[in_vmem(x) for x in (own, *coded)])


def on_device(user_factors, item_factors, user_tangent, item_tangent, block_mask, n_au, n_ia):
    us, width = user_factors.shape
    row_blocks, per = block_mask.shape
    per //= n_au
    members = us * n_ia // row_blocks // us
    assert members == 4
    scale = 1.0 / math.sqrt(width)
    core, near = 1, [0, 2, 4, 6]
    a_bits = bits_of(8, n_ia)
    rel_a = relative(a_bits)

    far = stack(user_factors, user_tangent)
    for bit in a_bits:
        far = jnp.concatenate([far, swap(far, "ia", n_ia, bit)], 0)

    item_bits = bits_of(1, n_au)
    rel_items = relative(item_bits)
    facs, tans = [item_factors[None]], [item_tangent[None]]
    for n, bit in enumerate(item_bits):
        held_f = facs[0] if n == 0 else jnp.concatenate(facs, 0)
        held_t = tans[0] if n == 0 else jnp.concatenate(tans, 0)
        facs.append(swap(held_f, "au", n_au, bit))
        tans.append(swap(held_t, "au", n_au, bit))
    rows = [(b ^ r) // members for b in near for r in rel_a]
    facs[0], tans[0], seen = load(
        block_mask, facs[0], tans[0], rows_of=(members, rows), cols_of=(per, rel_items), us=us, scale=scale
    )
    piece = len(rel_a) * us

    mine = [far] + [swap(far, "ia", n_ia, b) for b in near[1:]]
    other = [swap(x, "ia", n_ia, core) for x in mine]

    def call(users, g, sums, sums_at, item_sum, lanes=0):
        at = sum(f.shape[0] for f in facs[:g])
        return region(
            seen, users, (facs[g], tans[g]), sums, sums_at, item_sum, lanes=lanes, cols=(at, per), scale=scale
        )

    first, item_sum = call([mine[0], other[0]], 0, [], None, None)
    second, item_sum = call([mine[1], other[1], mine[2], other[2]], 0, [], None, item_sum)
    third, own_items = call([mine[3], other[3]], 0, [], None, item_sum, lanes=2 * piece)
    sums = [first, second, third]
    at_mine, at_other = [(0, 0), (1, 0), (1, 2), (2, 0)], [(0, 1), (1, 1), (1, 3), (2, 1)]
    item_sums = [own_items]
    for g in range(1, len(facs)):
        out_other, item_sum = call(other, g, sums, at_other, None)
        out_mine, item_sum = call(mine, g, sums, at_mine, item_sum)
        item_sums.append(item_sum)
        sums = [out_mine, out_other]
        at_mine, at_other = [(0, i) for i in range(4)], [(1, i) for i in range(4)]

    own, *coded = fold(out_mine, swap(out_other, "ia", n_ia, core))
    coded = [swap(q, "ia", n_ia, b) for q, b in zip(coded, near[1:])]
    acc, send = near_sum(own, coded)
    for n, bit in enumerate(a_bits[::-1]):
        if n:
            half = acc.shape[0] // 2
            acc, send = acc[:half], acc[half:]
        acc = acc + swap(send, "ia", n_ia, bit)
    user_product = acc.reshape(us, width)

    for bit in item_bits[::-1]:
        back = swap(encode(item_sums.pop()), "au", n_au, bit)
        sizes = [h.shape[0] for h in item_sums]
        cuts = [sum(sizes[:i]) for i in range(len(sizes))]
        item_sums = [add_decoded(h, back, c) for h, c in zip(item_sums, cuts)]
    item_product = item_sums[0][0]
    return user_product, item_product


def solution(mesh):
    n_au, n_ia = mesh.shape["au"], mesh.shape["ia"]
    placed = (
        P(("au", "ia"), None),
        P(("ia", "au"), None),
        P(("au", "ia"), None),
        P(("ia", "au"), None),
        P("au", "ia"),
    )

    def body(*args):
        return on_device(*args, n_au=n_au, n_ia=n_ia)

    return jax.shard_map(
        body,
        mesh=mesh,
        in_specs=placed,
        out_specs=(P(("au", "ia"), None), P(("ia", "au"), None)),
        check_vma=False,
    )
```

```python
import functools
import math

import jax
import jax.numpy as jnp
from jax import lax
from jax.experimental import pallas as pl
from jax.experimental.pallas import tpu as pltpu
from jax.sharding import PartitionSpec as P

f32 = jnp.float32
bf16 = jnp.bfloat16
NN = (((1,), (0,)), ((), ()))
NT = (((1,), (1,)), ((), ()))
TN = (((0,), (0,)), ((), ()))
dot = functools.partial(lax.dot_general, preferred_element_type=f32)
TILE = 256


def swap(x, axis, size, bits):
    return lax.ppermute(x, axis, [(i, i ^ bits) for i in range(size)])


def bits_of(low, high):
    out = []
    bit = high // 2
    while bit >= low:
        out.append(bit)
        bit //= 2
    return out


def relative(bits):
    order = [0]
    for bit in bits:
        order = order + [r ^ bit for r in order]
    return order


def region_kernel(*refs, n_users, sums_at, n_sums, add_item, lanes, cols, scale):
    seen_ref = refs[0]
    users = refs[1 : 1 + n_users]
    at = 1 + n_users
    fac_i, tan_i = refs[at : at + 2]
    at += 2
    user_in = refs[at : at + n_sums]
    at += n_sums
    item_in = refs[at] if add_item else None
    at += add_item
    user_out, item_out, u_all, c_all = refs[at:]

    n_a, _, us, _ = users[0].shape
    n_pieces, it_dev, _ = fac_i.shape
    for b, ref in enumerate(users):
        for k in range(n_a):
            for ft in range(2):
                u_all[ft, pl.ds((b * n_a + k) * us, us), :] = ref[k, ft]
    total_rows = n_users * n_a * us
    tile = min(TILE, total_rows)
    in_tile = tile // us
    blocks = cols[1]
    block = it_dev // blocks
    sub = min(TILE, it_dev)
    for t in range(total_rows // tile):
        rows = pl.ds(t * tile, tile)
        fac = u_all[0, rows, :]
        tan = u_all[1, rows, :]
        total = None
        for k in range(n_pieces):
            for ib in range(it_dev // sub):
                items = pl.ds(ib * sub, sub)
                v = fac_i[k, items, :]
                dv = tan_i[k, items, :]
                if 2 * tile <= TILE:
                    both = dot(v, jnp.concatenate([fac, tan], 0), NT)
                    s = both[:, :tile]
                    tt = both[:, tile:] + dot(dv, fac, NT)
                else:
                    s = dot(v, fac, NT)
                    tt = dot(v, tan, NT) + dot(dv, fac, NT)
                seen = []
                for i in range(sub // block):
                    row = seen_ref[
                        pl.ds((cols[0] + k) * blocks + ib * (sub // block) + i, 1), pl.ds(lanes + t * tile, tile)
                    ]
                    seen.append(jnp.broadcast_to(row, (block, tile)))
                seen = jnp.concatenate(seen, 0)
                e = jnp.exp(jnp.abs(s) * -scale)
                p = 1.0 / (1.0 + e)
                c = (e * p * p * (tt * seen)).astype(bf16)
                c_all[k, items, pl.ds(0, tile)] = c
            r = dot(c_all[k], fac, NN) * scale
            if t > 0:
                r = r + item_out[k]
            elif item_in is not None:
                r = r + item_in[k]
            item_out[k] = r
            part = dot(c_all[k], fac_i[k], TN)
            total = part if total is None else total + part
        total = total * scale
        for j in range(in_tile):
            b, k = divmod(t * in_tile + j, n_a)
            r = total[j * us : (j + 1) * us]
            if n_sums:
                r = r + user_in[sums_at[b][0]][sums_at[b][1], k]
            user_out[b, k] = r


def in_vmem(x):
    return pltpu.with_memory_space_constraint(x, pltpu.VMEM)


VM = pl.BlockSpec(memory_space=pltpu.VMEM)
PARAMS = pltpu.CompilerParams(vmem_limit_bytes=16 * 2**20)


def region(seen, users, items, sums, sums_at, item_sum, **static):
    n_a, _, us, width = users[0].shape
    n_pieces, it_dev, _ = items[0].shape
    given = [in_vmem(x) for x in (seen, *users, *items, *sums)]
    aliases = {}
    if item_sum is not None:
        aliases[len(given)] = 1
        given.append(in_vmem(item_sum))
    total_rows = len(users) * n_a * us
    return pl.pallas_call(
        functools.partial(
            region_kernel,
            n_users=len(users),
            sums_at=sums_at,
            n_sums=len(sums),
            add_item=item_sum is not None,
            **static,
        ),
        in_specs=[VM] * len(given),
        out_specs=[VM] * 2,
        out_shape=[
            pltpu.VMEM((len(users), n_a, us, width), f32),
            pltpu.VMEM((n_pieces, it_dev, width), f32),
        ],
        input_output_aliases=aliases,
        scratch_shapes=[
            pltpu.VMEM((2, total_rows, width), bf16),
            pltpu.VMEM((n_pieces, it_dev, min(TILE, total_rows)), bf16),
        ],
        compiler_params=PARAMS,
    )(*given)


def load_kernel(mask, fac, tan, fac_out, tan_out, seen, sems, *, rows_of, cols_of, us, scale):
    copies = [
        pltpu.make_async_copy(fac, fac_out, sems.at[0]),
        pltpu.make_async_copy(tan, tan_out, sems.at[1]),
    ]
    for c in copies:
        c.start()
    per, order = cols_of
    members, rows = rows_of
    me_row = lax.axis_index("ia") // members
    me_col = lax.axis_index("au")
    lane = lax.broadcasted_iota(jnp.int32, (1, seen.shape[1]), 1)
    for q, rel in enumerate(order):
        for i in range(per):
            value = {r: mask[me_row ^ r, (me_col ^ rel) * per + i].astype(f32) * scale for r in sorted(set(rows))}
            line = None
            for j in reversed(range(len(rows))):
                full = jnp.full(lane.shape, value[rows[j]], f32)
                line = full if line is None else jnp.where(lane < (j + 1) * us, full, line)
            seen[pl.ds(q * per + i, 1), :] = line
    for c in copies:
        c.wait()


def load(mask, fac, tan, **static):
    hbm = [pltpu.with_memory_space_constraint(x, pltpu.HBM) for x in (fac, tan)]
    blocks = static["cols_of"][0] * len(static["cols_of"][1])
    lanes = len(static["rows_of"][1]) * static["us"]
    return pl.pallas_call(
        functools.partial(load_kernel, **static),
        in_specs=[pl.BlockSpec(memory_space=pltpu.SMEM)] + [pl.BlockSpec(memory_space=pltpu.HBM)] * 2,
        out_specs=[VM] * 3,
        out_shape=[pltpu.VMEM(fac.shape, fac.dtype), pltpu.VMEM(tan.shape, tan.dtype), pltpu.VMEM((blocks, lanes), f32)],
        scratch_shapes=[pltpu.SemaphoreType.DMA((2,))],
        compiler_params=PARAMS,
    )(mask, *hbm)


def stack_kernel(a, b, out, sems):
    copies = [
        pltpu.make_async_copy(a, out.at[0, 0], sems.at[0]),
        pltpu.make_async_copy(b, out.at[0, 1], sems.at[1]),
    ]
    for c in copies:
        c.start()
    for c in copies:
        c.wait()


def stack(a, b):
    return pl.pallas_call(
        stack_kernel,
        in_specs=[pl.BlockSpec(memory_space=pltpu.HBM)] * 2,
        out_specs=VM,
        out_shape=pltpu.VMEM((1, 2, *a.shape), a.dtype),
        scratch_shapes=[pltpu.SemaphoreType.DMA((2,))],
        compiler_params=PARAMS,
    )(*[pltpu.with_memory_space_constraint(x, pltpu.HBM) for x in (a, b)])


GROUPS = 16


def encode_rows(x, out_ref, k):
    rows = x.shape[0]
    groups = min(GROUPS, rows // GROUPS)
    step = rows // groups
    exps = []
    for g in range(groups):
        part = x[g * step : (g + 1) * step]
        top = jnp.max(jnp.abs(part), 0, keepdims=True)
        e = 14.0 - jnp.ceil(jnp.log2(jnp.maximum(top, 1e-30)))
        out_ref[k, pl.ds(g * step, step), :] = jnp.round(part * jnp.exp2(e)).astype(jnp.int32).astype(jnp.int16)
        exps.append(e)
    exps += exps[-1:] * (GROUPS - groups)
    out_ref[k, pl.ds(rows, GROUPS), :] = jnp.concatenate(exps, 0).astype(jnp.int32).astype(jnp.int16)


def decode_rows(q_ref, k, g, groups):
    rows = q_ref.shape[1] - GROUPS
    step = rows // groups
    unit = jnp.exp2(-q_ref[k, pl.ds(rows, GROUPS), :].astype(jnp.int32).astype(f32))
    return q_ref[k, pl.ds(g * step, step), :].astype(jnp.int32).astype(f32) * unit[g : g + 1]


def encode_kernel(x_ref, out_ref):
    for k in range(x_ref.shape[0]):
        encode_rows(x_ref[k], out_ref, k)


def encode(x):
    n, rows, width = x.shape
    return pl.pallas_call(
        encode_kernel,
        in_specs=[VM],
        out_specs=VM,
        out_shape=pltpu.VMEM((n, rows + GROUPS, width), jnp.int16),
        compiler_params=PARAMS,
    )(in_vmem(x))


def decode_kernel(x_ref, q_ref, out_ref, *, at):
    n, rows, _ = x_ref.shape
    groups = min(GROUPS, rows // GROUPS)
    step = rows // groups
    for k in range(n):
        for g in range(groups):
            part = pl.ds(g * step, step)
            out_ref[k, part, :] = x_ref[k, part, :] + decode_rows(q_ref, at + k, g, groups)


def add_decoded(x, q, at):
    return pl.pallas_call(
        functools.partial(decode_kernel, at=at),
        in_specs=[VM, VM],
        out_specs=VM,
        out_shape=jax.ShapeDtypeStruct(x.shape, f32),
        compiler_params=PARAMS,
    )(in_vmem(x), in_vmem(q))


def decoded(q_ref, k):
    rows = q_ref.shape[1] - GROUPS
    groups = min(GROUPS, rows // GROUPS)
    return jnp.concatenate([decode_rows(q_ref, k, g, groups) for g in range(groups)], 0)


def fold_kernel(mine, core_in, keep, coded):
    n, n_a, us, width = mine.shape
    rows = n_a * us
    both = [(mine[i] + core_in[i]).reshape(rows, width) for i in range(n)]
    for i in range(0, n, 2):
        keep[i // 2] = both[i]
    encode_rows(jnp.concatenate(both[1::2], 0), coded, 0)


def fold(mine, core_in):
    n, n_a, us, width = mine.shape
    rows = n_a * us
    return pl.pallas_call(
        fold_kernel,
        in_specs=[VM, VM],
        out_specs=[VM] * 2,
        out_shape=[pltpu.VMEM((n // 2, rows, width), f32), pltpu.VMEM((1, n // 2 * rows + GROUPS, width), jnp.int16)],
        compiler_params=PARAMS,
    )(in_vmem(mine), in_vmem(core_in))


def spread_kernel(keep, q, own, *coded):
    n, rows, _ = keep.shape
    half = rows // 2
    came = decoded(q, 0)
    for i in range(n):
        x = keep[i] + came[i * rows : (i + 1) * rows]
        for j in range(2):
            part = x[j * half : (j + 1) * half]
            if i == 0 and j == 0:
                own[...] = part
            else:
                encode_rows(part, coded[2 * i + j - 1], 0)


def spread(keep, q):
    _, rows, width = keep.shape
    half = rows // 2
    return pl.pallas_call(
        spread_kernel,
        in_specs=[VM] * 2,
        out_specs=[VM] * 4,
        out_shape=[pltpu.VMEM((half, width), f32)] + [pltpu.VMEM((1, half + GROUPS, width), jnp.int16)] * 3,
        compiler_params=PARAMS,
    )(in_vmem(keep), in_vmem(q))


def total_kernel(own, *refs):
    x = own[...]
    for q in refs[:-1]:
        x = x + decoded(q, 0)
    refs[-1][...] = x


def total(own, coded):
    return pl.pallas_call(
        total_kernel,
        in_specs=[VM] * (1 + len(coded)),
        out_specs=VM,
        out_shape=jax.ShapeDtypeStruct(own.shape, f32),
        compiler_params=PARAMS,
    )(*[in_vmem(x) for x in (own, *coded)])


def on_device(user_factors, item_factors, user_tangent, item_tangent, block_mask, n_au, n_ia):
    us, width = user_factors.shape
    row_blocks, per = block_mask.shape
    per //= n_au
    members = us * n_ia // row_blocks // us
    assert members == 4
    scale = 1.0 / math.sqrt(width)
    core, near = 1, [0, 2, 4, 6]
    a_bits = bits_of(8, n_ia)
    rel_a = relative(a_bits)

    far = stack(user_factors, user_tangent)
    for bit in a_bits:
        far = jnp.concatenate([far, swap(far, "ia", n_ia, bit)], 0)

    item_bits = bits_of(1, n_au)
    rel_items = relative(item_bits)
    facs, tans = [item_factors[None]], [item_tangent[None]]
    for n, bit in enumerate(item_bits):
        held_f = facs[0] if n == 0 else jnp.concatenate(facs, 0)
        held_t = tans[0] if n == 0 else jnp.concatenate(tans, 0)
        facs.append(swap(held_f, "au", n_au, bit))
        tans.append(swap(held_t, "au", n_au, bit))
    rows = [(b ^ r) // members for b in near for r in rel_a]
    facs[0], tans[0], seen = load(
        block_mask, facs[0], tans[0], rows_of=(members, rows), cols_of=(per, rel_items), us=us, scale=scale
    )
    piece = len(rel_a) * us

    mine = [far] + [swap(far, "ia", n_ia, b) for b in near[1:]]
    other = [swap(x, "ia", n_ia, core) for x in mine]

    def call(users, g, sums, sums_at, item_sum, lanes=0):
        at = sum(f.shape[0] for f in facs[:g])
        return region(
            seen, users, (facs[g], tans[g]), sums, sums_at, item_sum, lanes=lanes, cols=(at, per), scale=scale
        )

    first, item_sum = call([mine[0], other[0]], 0, [], None, None)
    second, item_sum = call([mine[1], other[1], mine[2], other[2]], 0, [], None, item_sum)
    third, own_items = call([mine[3], other[3]], 0, [], None, item_sum, lanes=2 * piece)
    sums = [first, second, third]
    at_mine, at_other = [(0, 0), (1, 0), (1, 2), (2, 0)], [(0, 1), (1, 1), (1, 3), (2, 1)]
    item_sums = [own_items]
    for g in range(1, len(facs)):
        out_other, item_sum = call(other, g, sums, at_other, None)
        out_mine, item_sum = call(mine, g, sums, at_mine, item_sum)
        item_sums.append(item_sum)
        sums = [out_mine, out_other]
        at_mine, at_other = [(0, i) for i in range(4)], [(1, i) for i in range(4)]

    keep, odd = fold(out_mine, swap(out_other, "ia", n_ia, core))
    own, *coded = spread(keep, swap(odd, "ia", n_ia, near[1]))
    far_bit = a_bits[-1]
    coded = [swap(q, "ia", n_ia, b) for q, b in zip(coded, [far_bit, near[2], far_bit ^ near[2]])]
    acc = total(own, coded)
    for bit in a_bits[:-1][::-1]:
        half = acc.shape[0] // 2
        acc = acc[:half] + swap(acc[half:], "ia", n_ia, bit)
    user_product = acc.reshape(us, width)

    for bit in item_bits[::-1]:
        back = swap(encode(item_sums.pop()), "au", n_au, bit)
        sizes = [h.shape[0] for h in item_sums]
        cuts = [sum(sizes[:i]) for i in range(len(sizes))]
        item_sums = [add_decoded(h, back, c) for h, c in zip(item_sums, cuts)]
    item_product = item_sums[0][0]
    return user_product, item_product


def solution(mesh):
    n_au, n_ia = mesh.shape["au"], mesh.shape["ia"]
    placed = (
        P(("au", "ia"), None),
        P(("ia", "au"), None),
        P(("au", "ia"), None),
        P(("ia", "au"), None),
        P("au", "ia"),
    )

    def body(*args):
        return on_device(*args, n_au=n_au, n_ia=n_ia)

    return jax.shard_map(
        body,
        mesh=mesh,
        in_specs=placed,
        out_specs=(P(("au", "ia"), None), P(("ia", "au"), None)),
        check_vma=False,
    )
```

```python
import functools
import math

import jax
import jax.numpy as jnp
from jax import lax
from jax.experimental import pallas as pl
from jax.experimental.pallas import tpu as pltpu
from jax.sharding import PartitionSpec as P

f32 = jnp.float32
bf16 = jnp.bfloat16
NN = (((1,), (0,)), ((), ()))
NT = (((1,), (1,)), ((), ()))
TN = (((0,), (0,)), ((), ()))
dot = functools.partial(lax.dot_general, preferred_element_type=f32)
TILE = 256


def swap(x, axis, size, bits):
    return lax.ppermute(x, axis, [(i, i ^ bits) for i in range(size)])


def bits_of(low, high):
    out = []
    bit = high // 2
    while bit >= low:
        out.append(bit)
        bit //= 2
    return out


def relative(bits):
    order = [0]
    for bit in bits:
        order = order + [r ^ bit for r in order]
    return order


def region_kernel(*refs, n_users, sums_at, n_sums, add_item, lanes, cols, scale):
    seen_ref = refs[0]
    users = refs[1 : 1 + n_users]
    at = 1 + n_users
    fac_i, tan_i = refs[at : at + 2]
    at += 2
    user_in = refs[at : at + n_sums]
    at += n_sums
    item_in = refs[at] if add_item else None
    at += add_item
    user_out, item_out, u_all, c_all = refs[at:]

    n_a, _, us, _ = users[0].shape
    n_pieces, it_dev, _ = fac_i.shape
    for b, ref in enumerate(users):
        for k in range(n_a):
            for ft in range(2):
                u_all[ft, pl.ds((b * n_a + k) * us, us), :] = ref[k, ft]
    total_rows = n_users * n_a * us
    tile = min(TILE, total_rows)
    in_tile = tile // us
    blocks = cols[1]
    block = it_dev // blocks
    sub = min(TILE, it_dev)
    for t in range(total_rows // tile):
        rows = pl.ds(t * tile, tile)
        fac = u_all[0, rows, :]
        tan = u_all[1, rows, :]
        total = None
        for k in range(n_pieces):
            for ib in range(it_dev // sub):
                items = pl.ds(ib * sub, sub)
                v = fac_i[k, items, :]
                dv = tan_i[k, items, :]
                if 2 * tile <= TILE:
                    both = dot(v, jnp.concatenate([fac, tan], 0), NT)
                    s = both[:, :tile]
                    tt = both[:, tile:] + dot(dv, fac, NT)
                else:
                    s = dot(v, fac, NT)
                    tt = dot(v, tan, NT) + dot(dv, fac, NT)
                seen = []
                for i in range(sub // block):
                    row = seen_ref[
                        pl.ds((cols[0] + k) * blocks + ib * (sub // block) + i, 1), pl.ds(lanes + t * tile, tile)
                    ]
                    seen.append(jnp.broadcast_to(row, (block, tile)))
                seen = jnp.concatenate(seen, 0)
                e = jnp.exp(jnp.abs(s) * -scale)
                p = 1.0 / (1.0 + e)
                c = (e * p * p * (tt * seen)).astype(bf16)
                c_all[k, items, pl.ds(0, tile)] = c
            r = dot(c_all[k], fac, NN) * scale
            if t > 0:
                r = r + item_out[k]
            elif item_in is not None:
                r = r + item_in[k]
            item_out[k] = r
            part = dot(c_all[k], fac_i[k], TN)
            total = part if total is None else total + part
        total = total * scale
        for j in range(in_tile):
            b, k = divmod(t * in_tile + j, n_a)
            r = total[j * us : (j + 1) * us]
            if n_sums:
                r = r + user_in[sums_at[b][0]][sums_at[b][1], k]
            user_out[b, k] = r


def in_vmem(x):
    return pltpu.with_memory_space_constraint(x, pltpu.VMEM)


VM = pl.BlockSpec(memory_space=pltpu.VMEM)
PARAMS = pltpu.CompilerParams(vmem_limit_bytes=16 * 2**20)


def region(seen, users, items, sums, sums_at, item_sum, **static):
    n_a, _, us, width = users[0].shape
    n_pieces, it_dev, _ = items[0].shape
    given = [in_vmem(x) for x in (seen, *users, *items, *sums)]
    aliases = {}
    if item_sum is not None:
        aliases[len(given)] = 1
        given.append(in_vmem(item_sum))
    total_rows = len(users) * n_a * us
    return pl.pallas_call(
        functools.partial(
            region_kernel,
            n_users=len(users),
            sums_at=sums_at,
            n_sums=len(sums),
            add_item=item_sum is not None,
            **static,
        ),
        in_specs=[VM] * len(given),
        out_specs=[VM] * 2,
        out_shape=[
            pltpu.VMEM((len(users), n_a, us, width), f32),
            pltpu.VMEM((n_pieces, it_dev, width), f32),
        ],
        input_output_aliases=aliases,
        scratch_shapes=[
            pltpu.VMEM((2, total_rows, width), bf16),
            pltpu.VMEM((n_pieces, it_dev, min(TILE, total_rows)), bf16),
        ],
        compiler_params=PARAMS,
    )(*given)


def load_kernel(mask, fac, tan, fac_out, tan_out, seen, sems, *, rows_of, cols_of, us, scale):
    copies = [
        pltpu.make_async_copy(fac, fac_out, sems.at[0]),
        pltpu.make_async_copy(tan, tan_out, sems.at[1]),
    ]
    for c in copies:
        c.start()
    per, order = cols_of
    members, rows = rows_of
    me_row = lax.axis_index("ia") // members
    me_col = lax.axis_index("au")
    lane = lax.broadcasted_iota(jnp.int32, (1, seen.shape[1]), 1)
    for q, rel in enumerate(order):
        for i in range(per):
            value = {r: mask[me_row ^ r, (me_col ^ rel) * per + i].astype(f32) * scale for r in sorted(set(rows))}
            line = None
            for j in reversed(range(len(rows))):
                full = jnp.full(lane.shape, value[rows[j]], f32)
                line = full if line is None else jnp.where(lane < (j + 1) * us, full, line)
            seen[pl.ds(q * per + i, 1), :] = line
    for c in copies:
        c.wait()


def load(mask, fac, tan, **static):
    hbm = [pltpu.with_memory_space_constraint(x, pltpu.HBM) for x in (fac, tan)]
    blocks = static["cols_of"][0] * len(static["cols_of"][1])
    lanes = len(static["rows_of"][1]) * static["us"]
    return pl.pallas_call(
        functools.partial(load_kernel, **static),
        in_specs=[pl.BlockSpec(memory_space=pltpu.SMEM)] + [pl.BlockSpec(memory_space=pltpu.HBM)] * 2,
        out_specs=[VM] * 3,
        out_shape=[pltpu.VMEM(fac.shape, fac.dtype), pltpu.VMEM(tan.shape, tan.dtype), pltpu.VMEM((blocks, lanes), f32)],
        scratch_shapes=[pltpu.SemaphoreType.DMA((2,))],
        compiler_params=PARAMS,
    )(mask, *hbm)


def stack_kernel(a, b, out, sems):
    copies = [
        pltpu.make_async_copy(a, out.at[0, 0], sems.at[0]),
        pltpu.make_async_copy(b, out.at[0, 1], sems.at[1]),
    ]
    for c in copies:
        c.start()
    for c in copies:
        c.wait()


def stack(a, b):
    return pl.pallas_call(
        stack_kernel,
        in_specs=[pl.BlockSpec(memory_space=pltpu.HBM)] * 2,
        out_specs=VM,
        out_shape=pltpu.VMEM((1, 2, *a.shape), a.dtype),
        scratch_shapes=[pltpu.SemaphoreType.DMA((2,))],
        compiler_params=PARAMS,
    )(*[pltpu.with_memory_space_constraint(x, pltpu.HBM) for x in (a, b)])


GROUPS = 16


def encode_rows(x, out_ref, k):
    rows = x.shape[0]
    groups = min(GROUPS, rows // GROUPS)
    step = rows // groups
    exps = []
    for g in range(groups):
        part = x[g * step : (g + 1) * step]
        top = jnp.max(jnp.abs(part), 0, keepdims=True)
        e = 14.0 - jnp.ceil(jnp.log2(jnp.maximum(top, 1e-30)))
        out_ref[k, pl.ds(g * step, step), :] = jnp.round(part * jnp.exp2(e)).astype(jnp.int32).astype(jnp.int16)
        exps.append(e)
    exps += exps[-1:] * (GROUPS - groups)
    out_ref[k, pl.ds(rows, GROUPS), :] = jnp.concatenate(exps, 0).astype(jnp.int32).astype(jnp.int16)


def decode_rows(q_ref, k, g, groups):
    rows = q_ref.shape[1] - GROUPS
    step = rows // groups
    unit = jnp.exp2(-q_ref[k, pl.ds(rows, GROUPS), :].astype(jnp.int32).astype(f32))
    return q_ref[k, pl.ds(g * step, step), :].astype(jnp.int32).astype(f32) * unit[g : g + 1]


def encode_kernel(x_ref, out_ref):
    for k in range(x_ref.shape[0]):
        encode_rows(x_ref[k], out_ref, k)


def encode(x):
    n, rows, width = x.shape
    return pl.pallas_call(
        encode_kernel,
        in_specs=[VM],
        out_specs=VM,
        out_shape=pltpu.VMEM((n, rows + GROUPS, width), jnp.int16),
        compiler_params=PARAMS,
    )(in_vmem(x))


def decode_kernel(x_ref, q_ref, out_ref, buf, sems, *, at):
    n, rows, _ = x_ref.shape
    groups = min(GROUPS, rows // GROUPS)
    step = rows // groups
    parts = sems.shape[1]
    copies = []
    for k in range(n):
        for g in range(groups):
            part = pl.ds(g * step, step)
            buf[k, part, :] = x_ref[k, part, :] + decode_rows(q_ref, at + k, g, groups)
            if (g + 1) % (groups // parts) == 0:
                c = g // (groups // parts)
                done = pl.ds(c * (rows // parts), rows // parts)
                copies.append(pltpu.make_async_copy(buf.at[k, done], out_ref.at[k, done], sems.at[k, c]))
                copies[-1].start()
    for c in copies:
        c.wait()


def add_decoded(x, q, at):
    return pl.pallas_call(
        functools.partial(decode_kernel, at=at),
        in_specs=[VM, VM],
        out_specs=pl.BlockSpec(memory_space=pltpu.HBM),
        out_shape=jax.ShapeDtypeStruct(x.shape, f32),
        scratch_shapes=[pltpu.VMEM(x.shape, f32), pltpu.SemaphoreType.DMA((x.shape[0], 4))],
        compiler_params=PARAMS,
    )(in_vmem(x), in_vmem(q))


def decoded(q_ref, k):
    rows = q_ref.shape[1] - GROUPS
    groups = min(GROUPS, rows // GROUPS)
    return jnp.concatenate([decode_rows(q_ref, k, g, groups) for g in range(groups)], 0)


def fold_kernel(mine, core_in, keep, coded):
    n, n_a, us, width = mine.shape
    rows = n_a * us
    both = [(mine[i] + core_in[i]).reshape(rows, width) for i in range(n)]
    for i in range(0, n, 2):
        keep[i // 2] = both[i]
    encode_rows(jnp.concatenate(both[1::2], 0), coded, 0)


def fold(mine, core_in):
    n, n_a, us, width = mine.shape
    rows = n_a * us
    return pl.pallas_call(
        fold_kernel,
        in_specs=[VM, VM],
        out_specs=[VM] * 2,
        out_shape=[pltpu.VMEM((n // 2, rows, width), f32), pltpu.VMEM((1, n // 2 * rows + GROUPS, width), jnp.int16)],
        compiler_params=PARAMS,
    )(in_vmem(mine), in_vmem(core_in))


def spread_kernel(keep, q, own, *coded):
    n, rows, _ = keep.shape
    half = rows // 2
    came = decoded(q, 0)
    for i in range(n):
        x = keep[i] + came[i * rows : (i + 1) * rows]
        for j in range(2):
            part = x[j * half : (j + 1) * half]
            if i == 0 and j == 0:
                own[...] = part
            else:
                encode_rows(part, coded[2 * i + j - 1], 0)


def spread(keep, q):
    _, rows, width = keep.shape
    half = rows // 2
    return pl.pallas_call(
        spread_kernel,
        in_specs=[VM] * 2,
        out_specs=[VM] * 4,
        out_shape=[pltpu.VMEM((half, width), f32)] + [pltpu.VMEM((1, half + GROUPS, width), jnp.int16)] * 3,
        compiler_params=PARAMS,
    )(in_vmem(keep), in_vmem(q))


def total_kernel(own, *refs):
    x = own[...]
    for q in refs[:-1]:
        x = x + decoded(q, 0)
    refs[-1][...] = x


def total(own, coded):
    return pl.pallas_call(
        total_kernel,
        in_specs=[VM] * (1 + len(coded)),
        out_specs=VM,
        out_shape=jax.ShapeDtypeStruct(own.shape, f32),
        compiler_params=PARAMS,
    )(*[in_vmem(x) for x in (own, *coded)])


def on_device(user_factors, item_factors, user_tangent, item_tangent, block_mask, n_au, n_ia):
    us, width = user_factors.shape
    row_blocks, per = block_mask.shape
    per //= n_au
    members = us * n_ia // row_blocks // us
    assert members == 4
    scale = 1.0 / math.sqrt(width)
    core, near = 1, [0, 2, 4, 6]
    a_bits = bits_of(8, n_ia)
    rel_a = relative(a_bits)

    far = stack(user_factors, user_tangent)
    for bit in a_bits:
        far = jnp.concatenate([far, swap(far, "ia", n_ia, bit)], 0)

    item_bits = bits_of(1, n_au)
    rel_items = relative(item_bits)
    facs, tans = [item_factors[None]], [item_tangent[None]]
    for n, bit in enumerate(item_bits):
        held_f = facs[0] if n == 0 else jnp.concatenate(facs, 0)
        held_t = tans[0] if n == 0 else jnp.concatenate(tans, 0)
        facs.append(swap(held_f, "au", n_au, bit))
        tans.append(swap(held_t, "au", n_au, bit))
    rows = [(b ^ r) // members for b in near for r in rel_a]
    facs[0], tans[0], seen = load(
        block_mask, facs[0], tans[0], rows_of=(members, rows), cols_of=(per, rel_items), us=us, scale=scale
    )
    piece = len(rel_a) * us

    mine = [far] + [swap(far, "ia", n_ia, b) for b in near[1:]]
    other = [swap(x, "ia", n_ia, core) for x in mine]

    def call(users, g, sums, sums_at, item_sum, lanes=0):
        at = sum(f.shape[0] for f in facs[:g])
        return region(
            seen, users, (facs[g], tans[g]), sums, sums_at, item_sum, lanes=lanes, cols=(at, per), scale=scale
        )

    first, item_sum = call([mine[0], other[0]], 0, [], None, None)
    second, item_sum = call([mine[1], other[1], mine[2], other[2]], 0, [], None, item_sum)
    third, own_items = call([mine[3], other[3]], 0, [], None, item_sum, lanes=2 * piece)
    sums = [first, second, third]
    at_mine, at_other = [(0, 0), (1, 0), (1, 2), (2, 0)], [(0, 1), (1, 1), (1, 3), (2, 1)]
    item_sums = [own_items]
    for g in range(1, len(facs)):
        out_other, item_sum = call(other, g, sums, at_other, None)
        out_mine, item_sum = call(mine, g, sums, at_mine, item_sum)
        item_sums.append(item_sum)
        sums = [out_mine, out_other]
        at_mine, at_other = [(0, i) for i in range(4)], [(1, i) for i in range(4)]

    keep, odd = fold(out_mine, swap(out_other, "ia", n_ia, core))
    own, *coded = spread(keep, swap(odd, "ia", n_ia, near[1]))
    far_bit = a_bits[-1]
    coded = [swap(q, "ia", n_ia, b) for q, b in zip(coded, [far_bit, near[2], far_bit ^ near[2]])]
    acc = total(own, coded)
    for bit in a_bits[:-1][::-1]:
        half = acc.shape[0] // 2
        acc = acc[:half] + swap(acc[half:], "ia", n_ia, bit)
    user_product = acc.reshape(us, width)

    for bit in item_bits[::-1]:
        back = swap(encode(item_sums.pop()), "au", n_au, bit)
        sizes = [h.shape[0] for h in item_sums]
        cuts = [sum(sizes[:i]) for i in range(len(sizes))]
        item_sums = [add_decoded(h, back, c) for h, c in zip(item_sums, cuts)]
    item_product = item_sums[0][0]
    return user_product, item_product


def solution(mesh):
    n_au, n_ia = mesh.shape["au"], mesh.shape["ia"]
    placed = (
        P(("au", "ia"), None),
        P(("ia", "au"), None),
        P(("au", "ia"), None),
        P(("ia", "au"), None),
        P("au", "ia"),
    )

    def body(*args):
        return on_device(*args, n_au=n_au, n_ia=n_ia)

    return jax.shard_map(
        body,
        mesh=mesh,
        in_specs=placed,
        out_specs=(P(("au", "ia"), None), P(("ia", "au"), None)),
        check_vma=False,
    )
```

```python
import functools
import math

import jax
import jax.numpy as jnp
from jax import lax
from jax.experimental import pallas as pl
from jax.experimental.pallas import tpu as pltpu
from jax.sharding import PartitionSpec as P

f32 = jnp.float32
bf16 = jnp.bfloat16
NN = (((1,), (0,)), ((), ()))
NT = (((1,), (1,)), ((), ()))
TN = (((0,), (0,)), ((), ()))
dot = functools.partial(lax.dot_general, preferred_element_type=f32)
TILE = 256


def swap(x, axis, size, bits):
    return lax.ppermute(x, axis, [(i, i ^ bits) for i in range(size)])


def bits_of(low, high):
    out = []
    bit = high // 2
    while bit >= low:
        out.append(bit)
        bit //= 2
    return out


def relative(bits):
    order = [0]
    for bit in bits:
        order = order + [r ^ bit for r in order]
    return order


def spread_seen(seen_ref, at, n, block, lanes, tile):
    rows = [jnp.broadcast_to(seen_ref[pl.ds(at + i, 1), pl.ds(lanes, tile)], (block, tile)) for i in range(n)]
    return jnp.concatenate(rows, 0)


def region_kernel(*refs, n_users, sums_at, n_sums, add_item, lanes, cols, scale, prepared):
    seen_ref = refs[0]
    users = refs[1 : 1 + n_users]
    at = 1 + n_users
    fac_i, tan_i = refs[at : at + 2]
    at += 2
    user_in = refs[at : at + n_sums]
    at += n_sums
    item_in = refs[at] if add_item else None
    at += add_item
    ready = None
    if prepared is not None:
        ready = refs[at : at + 2]
        at += 2
    user_out, item_out, u_all, c_all = refs[at:]

    n_a, _, us, _ = users[0].shape
    n_pieces, it_dev, _ = fac_i.shape
    for b, ref in enumerate(users):
        for k in range(n_a):
            for ft in range(2):
                u_all[ft, pl.ds((b * n_a + k) * us, us), :] = ref[k, ft]
    total_rows = n_users * n_a * us
    tile = min(TILE, total_rows)
    in_tile = tile // us
    blocks = cols[1]
    block = it_dev // blocks
    sub = min(TILE, it_dev)
    for t in range(total_rows // tile):
        rows = pl.ds(t * tile, tile)
        fac = u_all[0, rows, :]
        tan = u_all[1, rows, :]
        total = None
        for k in range(n_pieces):
            for ib in range(it_dev // sub):
                items = pl.ds(ib * sub, sub)
                v = fac_i[k, items, :]
                dv = tan_i[k, items, :]
                if ready is not None:
                    weight, tt = (x[prepared + t, items, :] for x in ready)
                    c = (weight * (tt + dot(dv, fac, NT))).astype(bf16)
                    c_all[k, items, pl.ds(0, tile)] = c
                    continue
                if 2 * tile <= TILE:
                    both = dot(v, jnp.concatenate([fac, tan], 0), NT)
                    s = both[:, :tile]
                    tt = both[:, tile:] + dot(dv, fac, NT)
                else:
                    s = dot(v, fac, NT)
                    tt = dot(v, tan, NT) + dot(dv, fac, NT)
                at_col = (cols[0] + k) * blocks + ib * (sub // block)
                seen = spread_seen(seen_ref, at_col, sub // block, block, lanes + t * tile, tile)
                e = jnp.exp(jnp.abs(s) * -scale)
                p = 1.0 / (1.0 + e)
                c = (e * p * p * (tt * seen)).astype(bf16)
                c_all[k, items, pl.ds(0, tile)] = c
            r = dot(c_all[k], fac, NN) * scale
            if t > 0:
                r = r + item_out[k]
            elif item_in is not None:
                r = r + item_in[k]
            item_out[k] = r
            part = dot(c_all[k], fac_i[k], TN)
            total = part if total is None else total + part
        total = total * scale
        for j in range(in_tile):
            b, k = divmod(t * in_tile + j, n_a)
            r = total[j * us : (j + 1) * us]
            if n_sums:
                r = r + user_in[sums_at[b][0]][sums_at[b][1], k]
            user_out[b, k] = r


def prepare_kernel(*refs, n_users, cols, scale):
    seen_ref = refs[0]
    users = refs[1 : 1 + n_users]
    fac_i, weight, part, u_all = refs[1 + n_users :]
    n_a, _, us, _ = users[0].shape
    tile = weight.shape[2]
    it_dev = fac_i.shape[1]
    block = it_dev // cols[1]
    for b, ref in enumerate(users):
        for k in range(n_a):
            for ft in range(2):
                u_all[ft, pl.ds((b * n_a + k) * us, us), :] = ref[k, ft]
    sub = min(TILE, it_dev)
    for t in range(weight.shape[0]):
        fac = u_all[0, pl.ds(t * tile, tile), :]
        tan = u_all[1, pl.ds(t * tile, tile), :]
        for ib in range(it_dev // sub):
            items = pl.ds(ib * sub, sub)
            v = fac_i[0, items, :]
            s = dot(v, fac, NT)
            part[t, items, :] = dot(v, tan, NT)
            at_col = cols[0] * cols[1] + ib * (sub // block)
            seen = spread_seen(seen_ref, at_col, sub // block, block, t * tile % seen_ref.shape[1], tile)
            e = jnp.exp(jnp.abs(s) * -scale)
            p = 1.0 / (1.0 + e)
            weight[t, items, :] = e * p * p * seen


def in_vmem(x):
    return pltpu.with_memory_space_constraint(x, pltpu.VMEM)


VM = pl.BlockSpec(memory_space=pltpu.VMEM)
PARAMS = pltpu.CompilerParams(vmem_limit_bytes=16 * 2**20)


def region(seen, users, items, sums, sums_at, item_sum, ready=(), prepared=None, **static):
    n_a, _, us, width = users[0].shape
    n_pieces, it_dev, _ = items[0].shape
    given = [in_vmem(x) for x in (seen, *users, *items, *sums)]
    aliases = {}
    if item_sum is not None:
        aliases[len(given)] = 1
        given.append(in_vmem(item_sum))
    given += [in_vmem(x) for x in ready]
    total_rows = len(users) * n_a * us
    return pl.pallas_call(
        functools.partial(
            region_kernel,
            n_users=len(users),
            sums_at=sums_at,
            n_sums=len(sums),
            add_item=item_sum is not None,
            prepared=prepared,
            **static,
        ),
        in_specs=[VM] * len(given),
        out_specs=[VM] * 2,
        out_shape=[
            pltpu.VMEM((len(users), n_a, us, width), f32),
            pltpu.VMEM((n_pieces, it_dev, width), f32),
        ],
        input_output_aliases=aliases,
        scratch_shapes=[
            pltpu.VMEM((2, total_rows, width), bf16),
            pltpu.VMEM((n_pieces, it_dev, min(TILE, total_rows)), bf16),
        ],
        compiler_params=PARAMS,
    )(*given)


def prepare(seen, users, fac, **static):
    n_a, _, us, width = users[0].shape
    rows = len(users) * n_a * us
    tile = min(TILE, rows // 2)
    shape = (rows // tile, fac.shape[1], tile)
    return pl.pallas_call(
        functools.partial(prepare_kernel, n_users=len(users), **static),
        in_specs=[VM] * (2 + len(users)),
        out_specs=[VM] * 2,
        out_shape=[pltpu.VMEM(shape, f32)] * 2,
        scratch_shapes=[pltpu.VMEM((2, rows, width), bf16)],
        compiler_params=PARAMS,
    )(*[in_vmem(x) for x in (seen, *users, fac)])


def load_kernel(mask, fac, tan, fac_out, tan_out, seen, sems, *, rows_of, cols_of, us, scale):
    copies = [
        pltpu.make_async_copy(fac, fac_out, sems.at[0]),
        pltpu.make_async_copy(tan, tan_out, sems.at[1]),
    ]
    for c in copies:
        c.start()
    per, order = cols_of
    members, rows = rows_of
    me_row = lax.axis_index("ia") // members
    me_col = lax.axis_index("au")
    lane = lax.broadcasted_iota(jnp.int32, (1, seen.shape[1]), 1)
    col = lax.broadcasted_iota(jnp.int32, (1, mask.shape[1]), 1)
    lines = {r: mask[pl.ds(me_row ^ r, 1), :].astype(f32) * scale for r in sorted(set(rows))}
    for q, rel in enumerate(order):
        for i in range(per):
            here = col == (me_col ^ rel) * per + i
            value = {r: jnp.sum(jnp.where(here, x, 0.0), 1, keepdims=True) for r, x in lines.items()}
            line = None
            for j in reversed(range(len(rows))):
                full = jnp.broadcast_to(value[rows[j]], lane.shape)
                line = full if line is None else jnp.where(lane < (j + 1) * us, full, line)
            seen[pl.ds(q * per + i, 1), :] = line
    for c in copies:
        c.wait()


def load(mask, fac, tan, **static):
    hbm = [pltpu.with_memory_space_constraint(x, pltpu.HBM) for x in (fac, tan)]
    blocks = static["cols_of"][0] * len(static["cols_of"][1])
    lanes = len(static["rows_of"][1]) * static["us"]
    return pl.pallas_call(
        functools.partial(load_kernel, **static),
        in_specs=[VM] + [pl.BlockSpec(memory_space=pltpu.HBM)] * 2,
        out_specs=[VM] * 3,
        out_shape=[pltpu.VMEM(fac.shape, fac.dtype), pltpu.VMEM(tan.shape, tan.dtype), pltpu.VMEM((blocks, lanes), f32)],
        scratch_shapes=[pltpu.SemaphoreType.DMA((2,))],
        compiler_params=PARAMS,
    )(in_vmem(mask), *hbm)


def stack_kernel(a, b, out, sems):
    copies = [
        pltpu.make_async_copy(a, out.at[0, 0], sems.at[0]),
        pltpu.make_async_copy(b, out.at[0, 1], sems.at[1]),
    ]
    for c in copies:
        c.start()
    for c in copies:
        c.wait()


def stack(a, b):
    return pl.pallas_call(
        stack_kernel,
        in_specs=[pl.BlockSpec(memory_space=pltpu.HBM)] * 2,
        out_specs=VM,
        out_shape=pltpu.VMEM((1, 2, *a.shape), a.dtype),
        scratch_shapes=[pltpu.SemaphoreType.DMA((2,))],
        compiler_params=PARAMS,
    )(*[pltpu.with_memory_space_constraint(x, pltpu.HBM) for x in (a, b)])


GROUPS = 16


def encode_rows(x, out_ref, k):
    rows = x.shape[0]
    groups = min(GROUPS, rows // GROUPS)
    step = rows // groups
    exps = []
    for g in range(groups):
        part = x[g * step : (g + 1) * step]
        top = jnp.max(jnp.abs(part), 0, keepdims=True)
        e = 14.0 - jnp.ceil(jnp.log2(jnp.maximum(top, 1e-30)))
        out_ref[k, pl.ds(g * step, step), :] = jnp.round(part * jnp.exp2(e)).astype(jnp.int32).astype(jnp.int16)
        exps.append(e)
    exps += exps[-1:] * (GROUPS - groups)
    out_ref[k, pl.ds(rows, GROUPS), :] = jnp.concatenate(exps, 0).astype(jnp.int32).astype(jnp.int16)


def decode_rows(q_ref, k, g, groups):
    rows = q_ref.shape[1] - GROUPS
    step = rows // groups
    unit = jnp.exp2(-q_ref[k, pl.ds(rows, GROUPS), :].astype(jnp.int32).astype(f32))
    return q_ref[k, pl.ds(g * step, step), :].astype(jnp.int32).astype(f32) * unit[g : g + 1]


def encode_kernel(x_ref, out_ref):
    for k in range(x_ref.shape[0]):
        encode_rows(x_ref[k], out_ref, k)


def encode(x):
    n, rows, width = x.shape
    return pl.pallas_call(
        encode_kernel,
        in_specs=[VM],
        out_specs=VM,
        out_shape=pltpu.VMEM((n, rows + GROUPS, width), jnp.int16),
        compiler_params=PARAMS,
    )(in_vmem(x))


def decode_kernel(x_ref, q_ref, out_ref, buf, sems, *, at):
    n, rows, _ = x_ref.shape
    groups = min(GROUPS, rows // GROUPS)
    step = rows // groups
    parts = sems.shape[1]
    copies = []
    for k in range(n):
        for g in range(groups):
            part = pl.ds(g * step, step)
            buf[k, part, :] = x_ref[k, part, :] + decode_rows(q_ref, at + k, g, groups)
            if (g + 1) % (groups // parts) == 0:
                c = g // (groups // parts)
                done = pl.ds(c * (rows // parts), rows // parts)
                copies.append(pltpu.make_async_copy(buf.at[k, done], out_ref.at[k, done], sems.at[k, c]))
                copies[-1].start()
    for c in copies:
        c.wait()


def add_decoded(x, q, at):
    return pl.pallas_call(
        functools.partial(decode_kernel, at=at),
        in_specs=[VM, VM],
        out_specs=pl.BlockSpec(memory_space=pltpu.HBM),
        out_shape=jax.ShapeDtypeStruct(x.shape, f32),
        scratch_shapes=[pltpu.VMEM(x.shape, f32), pltpu.SemaphoreType.DMA((x.shape[0], 4))],
        compiler_params=PARAMS,
    )(in_vmem(x), in_vmem(q))


def decoded(q_ref, k):
    rows = q_ref.shape[1] - GROUPS
    groups = min(GROUPS, rows // GROUPS)
    return jnp.concatenate([decode_rows(q_ref, k, g, groups) for g in range(groups)], 0)


def fold_kernel(mine, core_in, keep, coded):
    n, n_a, us, width = mine.shape
    rows = n_a * us
    both = [(mine[i] + core_in[i]).reshape(rows, width) for i in range(n)]
    for i in range(0, n, 2):
        keep[i // 2] = both[i]
    encode_rows(jnp.concatenate(both[1::2], 0), coded, 0)


def fold(mine, core_in):
    n, n_a, us, width = mine.shape
    rows = n_a * us
    return pl.pallas_call(
        fold_kernel,
        in_specs=[VM, VM],
        out_specs=[VM] * 2,
        out_shape=[pltpu.VMEM((n // 2, rows, width), f32), pltpu.VMEM((1, n // 2 * rows + GROUPS, width), jnp.int16)],
        compiler_params=PARAMS,
    )(in_vmem(mine), in_vmem(core_in))


def spread_kernel(keep, q, own, *coded):
    n, rows, _ = keep.shape
    half = rows // 2
    came = decoded(q, 0)
    for i in range(n):
        x = keep[i] + came[i * rows : (i + 1) * rows]
        for j in range(2):
            part = x[j * half : (j + 1) * half]
            if i == 0 and j == 0:
                own[...] = part
            else:
                encode_rows(part, coded[2 * i + j - 1], 0)


def spread(keep, q):
    _, rows, width = keep.shape
    half = rows // 2
    return pl.pallas_call(
        spread_kernel,
        in_specs=[VM] * 2,
        out_specs=[VM] * 4,
        out_shape=[pltpu.VMEM((half, width), f32)] + [pltpu.VMEM((1, half + GROUPS, width), jnp.int16)] * 3,
        compiler_params=PARAMS,
    )(in_vmem(keep), in_vmem(q))


def total_kernel(own, *refs):
    x = own[...]
    for q in refs[:-1]:
        x = x + decoded(q, 0)
    refs[-1][...] = x


def total(own, coded):
    return pl.pallas_call(
        total_kernel,
        in_specs=[VM] * (1 + len(coded)),
        out_specs=VM,
        out_shape=jax.ShapeDtypeStruct(own.shape, f32),
        compiler_params=PARAMS,
    )(*[in_vmem(x) for x in (own, *coded)])


def on_device(user_factors, item_factors, user_tangent, item_tangent, block_mask, n_au, n_ia):
    us, width = user_factors.shape
    row_blocks, per = block_mask.shape
    per //= n_au
    members = us * n_ia // row_blocks // us
    assert members == 4
    scale = 1.0 / math.sqrt(width)
    core, near = 1, [0, 2, 4, 6]
    a_bits = bits_of(8, n_ia)
    rel_a = relative(a_bits)

    far = stack(user_factors, user_tangent)
    for bit in a_bits:
        far = jnp.concatenate([far, swap(far, "ia", n_ia, bit)], 0)

    item_bits = bits_of(1, n_au)
    rel_items = relative(item_bits)
    facs, tans = [item_factors[None]], [item_tangent[None]]
    for n, bit in enumerate(item_bits):
        held_f = facs[0] if n == 0 else jnp.concatenate(facs, 0)
        held_t = tans[0] if n == 0 else jnp.concatenate(tans, 0)
        facs.append(swap(held_f, "au", n_au, bit))
        tans.append(swap(held_t, "au", n_au, bit))
    rows = [(b ^ r) // members for b in near for r in rel_a]
    facs[0], tans[0], seen = load(
        block_mask, facs[0], tans[0], rows_of=(members, rows), cols_of=(per, rel_items), us=us, scale=scale
    )
    piece = len(rel_a) * us

    mine = [far] + [swap(far, "ia", n_ia, b) for b in near[1:]]
    other = [swap(x, "ia", n_ia, core) for x in mine]

    def call(users, g, sums, sums_at, item_sum, lanes=0, **extra):
        at = sum(f.shape[0] for f in facs[:g])
        return region(
            seen, users, (facs[g], tans[g]), sums, sums_at, item_sum, lanes=lanes, cols=(at, per), scale=scale, **extra
        )

    first, item_sum = call([mine[0], other[0]], 0, [], None, None)
    second, item_sum = call([mine[1], other[1], mine[2], other[2]], 0, [], None, item_sum)
    third, own_items = call([mine[3], other[3]], 0, [], None, item_sum, lanes=2 * piece)
    sums = [first, second, third]
    at_mine, at_other = [(0, 0), (1, 0), (1, 2), (2, 0)], [(0, 1), (1, 1), (1, 3), (2, 1)]
    item_sums = [own_items]
    for g in range(1, len(facs)):
        first, second = {}, {}
        if facs[g].shape[0] == 1:
            ready = prepare(seen, [*other, *mine], facs[g], cols=(g, per), scale=scale)
            first = {"ready": ready, "prepared": 0}
            second = {"ready": ready, "prepared": ready[0].shape[0] // 2}
        out_other, item_sum = call(other, g, sums, at_other, None, **first)
        out_mine, item_sum = call(mine, g, sums, at_mine, item_sum, **second)
        item_sums.append(item_sum)
        sums = [out_mine, out_other]
        at_mine, at_other = [(0, i) for i in range(4)], [(1, i) for i in range(4)]

    keep, odd = fold(out_mine, swap(out_other, "ia", n_ia, core))
    own, *coded = spread(keep, swap(odd, "ia", n_ia, near[1]))
    far_bit = a_bits[-1]
    coded = [swap(q, "ia", n_ia, b) for q, b in zip(coded, [far_bit, near[2], far_bit ^ near[2]])]
    acc = total(own, coded)
    for bit in a_bits[:-1][::-1]:
        half = acc.shape[0] // 2
        acc = acc[:half] + swap(acc[half:], "ia", n_ia, bit)
    user_product = acc.reshape(us, width)

    for bit in item_bits[::-1]:
        back = swap(encode(item_sums.pop()), "au", n_au, bit)
        sizes = [h.shape[0] for h in item_sums]
        cuts = [sum(sizes[:i]) for i in range(len(sizes))]
        item_sums = [add_decoded(h, back, c) for h, c in zip(item_sums, cuts)]
    item_product = item_sums[0][0]
    return user_product, item_product


def solution(mesh):
    n_au, n_ia = mesh.shape["au"], mesh.shape["ia"]
    placed = (
        P(("au", "ia"), None),
        P(("ia", "au"), None),
        P(("au", "ia"), None),
        P(("ia", "au"), None),
        P("au", "ia"),
    )

    def body(*args):
        return on_device(*args, n_au=n_au, n_ia=n_ia)

    return jax.shard_map(
        body,
        mesh=mesh,
        in_specs=placed,
        out_specs=(P(("au", "ia"), None), P(("ia", "au"), None)),
        check_vma=False,
    )
```

```python
import functools
import math

import jax
import jax.numpy as jnp
from jax import lax
from jax.experimental import pallas as pl
from jax.experimental.pallas import tpu as pltpu
from jax.sharding import PartitionSpec as P

f32 = jnp.float32
bf16 = jnp.bfloat16
NN = (((1,), (0,)), ((), ()))
NT = (((1,), (1,)), ((), ()))
TN = (((0,), (0,)), ((), ()))
dot = functools.partial(lax.dot_general, preferred_element_type=f32)
TILE = 256


def swap(x, axis, size, bits):
    return lax.ppermute(x, axis, [(i, i ^ bits) for i in range(size)])


def bits_of(low, high):
    out = []
    bit = high // 2
    while bit >= low:
        out.append(bit)
        bit //= 2
    return out


def relative(bits):
    order = [0]
    for bit in bits:
        order = order + [r ^ bit for r in order]
    return order


def spread_seen(seen_ref, at, n, block, lanes, tile):
    rows = [jnp.broadcast_to(seen_ref[pl.ds(at + i, 1), pl.ds(lanes, tile)], (block, tile)) for i in range(n)]
    return jnp.concatenate(rows, 0)


def region_kernel(*refs, n_users, sums_at, n_sums, add_item, lanes, cols, scale, prepared):
    seen_ref = refs[0]
    users = refs[1 : 1 + n_users]
    at = 1 + n_users
    fac_i, tan_i = refs[at : at + 2]
    at += 2
    user_in = refs[at : at + n_sums]
    at += n_sums
    item_in = refs[at] if add_item else None
    at += add_item
    ready = None
    if prepared is not None:
        ready = refs[at : at + 2]
        at += 2
    user_out, item_out, u_all, c_all = refs[at:]

    n_a, _, us, _ = users[0].shape
    n_pieces, it_dev, _ = fac_i.shape
    for b, ref in enumerate(users):
        for k in range(n_a):
            for ft in range(2):
                u_all[ft, pl.ds((b * n_a + k) * us, us), :] = ref[k, ft]
    total_rows = n_users * n_a * us
    tile = min(TILE, total_rows)
    in_tile = tile // us
    blocks = cols[1]
    block = it_dev // blocks
    sub = min(TILE, it_dev)
    for t in range(total_rows // tile):
        rows = pl.ds(t * tile, tile)
        fac = u_all[0, rows, :]
        tan = u_all[1, rows, :]
        total = None
        for k in range(n_pieces):
            for ib in range(it_dev // sub):
                items = pl.ds(ib * sub, sub)
                v = fac_i[k, items, :]
                dv = tan_i[k, items, :]
                if ready is not None:
                    weight, tt = (x[prepared + t, items, :] for x in ready)
                    c = (weight * (tt + dot(dv, fac, NT))).astype(bf16)
                    c_all[k, items, pl.ds(0, tile)] = c
                    continue
                if 2 * tile <= TILE:
                    both = dot(v, jnp.concatenate([fac, tan], 0), NT)
                    s = both[:, :tile]
                    tt = both[:, tile:] + dot(dv, fac, NT)
                else:
                    s = dot(v, fac, NT)
                    tt = dot(v, tan, NT) + dot(dv, fac, NT)
                at_col = (cols[0] + k) * blocks + ib * (sub // block)
                seen = spread_seen(seen_ref, at_col, sub // block, block, lanes + t * tile, tile)
                e = jnp.exp(jnp.abs(s) * -scale)
                p = 1.0 / (1.0 + e)
                c = (e * p * p * (tt * seen)).astype(bf16)
                c_all[k, items, pl.ds(0, tile)] = c
            r = dot(c_all[k], fac, NN) * scale
            if t > 0:
                r = r + item_out[k]
            elif item_in is not None:
                r = r + item_in[k]
            item_out[k] = r
            part = dot(c_all[k], fac_i[k], TN)
            total = part if total is None else total + part
        total = total * scale
        for j in range(in_tile):
            b, k = divmod(t * in_tile + j, n_a)
            r = total[j * us : (j + 1) * us]
            if n_sums:
                r = r + user_in[sums_at[b][0]][sums_at[b][1], k]
            user_out[b, k] = r


def prepare_kernel(*refs, n_users, lanes, cols, scale):
    seen_ref = refs[0]
    users = refs[1 : 1 + n_users]
    fac_i, weight, part, u_all = refs[1 + n_users :]
    n_a, _, us, _ = users[0].shape
    tile = weight.shape[2]
    it_dev = fac_i.shape[1]
    block = it_dev // cols[1]
    for b, ref in enumerate(users):
        for k in range(n_a):
            for ft in range(2):
                u_all[ft, pl.ds((b * n_a + k) * us, us), :] = ref[k, ft]
    sub = min(TILE, it_dev)
    for t in range(weight.shape[0]):
        fac = u_all[0, pl.ds(t * tile, tile), :]
        tan = u_all[1, pl.ds(t * tile, tile), :]
        for ib in range(it_dev // sub):
            items = pl.ds(ib * sub, sub)
            v = fac_i[0, items, :]
            s = dot(v, fac, NT)
            part[t, items, :] = dot(v, tan, NT)
            at_col = cols[0] * cols[1] + ib * (sub // block)
            seen = spread_seen(seen_ref, at_col, sub // block, block, lanes + t * tile % (seen_ref.shape[1] - lanes), tile)
            e = jnp.exp(jnp.abs(s) * -scale)
            p = 1.0 / (1.0 + e)
            weight[t, items, :] = e * p * p * seen


def in_vmem(x):
    return pltpu.with_memory_space_constraint(x, pltpu.VMEM)


VM = pl.BlockSpec(memory_space=pltpu.VMEM)
PARAMS = pltpu.CompilerParams(vmem_limit_bytes=16 * 2**20)


def region(seen, users, items, sums, sums_at, item_sum, ready=(), prepared=None, **static):
    n_a, _, us, width = users[0].shape
    n_pieces, it_dev, _ = items[0].shape
    given = [in_vmem(x) for x in (seen, *users, *items, *sums)]
    aliases = {}
    if item_sum is not None:
        aliases[len(given)] = 1
        given.append(in_vmem(item_sum))
    given += [in_vmem(x) for x in ready]
    total_rows = len(users) * n_a * us
    return pl.pallas_call(
        functools.partial(
            region_kernel,
            n_users=len(users),
            sums_at=sums_at,
            n_sums=len(sums),
            add_item=item_sum is not None,
            prepared=prepared,
            **static,
        ),
        in_specs=[VM] * len(given),
        out_specs=[VM] * 2,
        out_shape=[
            pltpu.VMEM((len(users), n_a, us, width), f32),
            pltpu.VMEM((n_pieces, it_dev, width), f32),
        ],
        input_output_aliases=aliases,
        scratch_shapes=[
            pltpu.VMEM((2, total_rows, width), bf16),
            pltpu.VMEM((n_pieces, it_dev, min(TILE, total_rows)), bf16),
        ],
        compiler_params=PARAMS,
    )(*given)


def prepare(seen, users, fac, **static):
    n_a, _, us, width = users[0].shape
    rows = len(users) * n_a * us
    tile = min(TILE, rows // 2)
    shape = (rows // tile, fac.shape[1], tile)
    return pl.pallas_call(
        functools.partial(prepare_kernel, n_users=len(users), **static),
        in_specs=[VM] * (2 + len(users)),
        out_specs=[VM] * 2,
        out_shape=[pltpu.VMEM(shape, f32)] * 2,
        scratch_shapes=[pltpu.VMEM((2, rows, width), bf16)],
        compiler_params=PARAMS,
    )(*[in_vmem(x) for x in (seen, *users, fac)])


def load_kernel(mask, fac, tan, fac_out, tan_out, seen, sems, *, rows_of, cols_of, us, scale):
    copies = [
        pltpu.make_async_copy(fac, fac_out, sems.at[0]),
        pltpu.make_async_copy(tan, tan_out, sems.at[1]),
    ]
    for c in copies:
        c.start()
    per, order = cols_of
    members, rows = rows_of
    me_row = lax.axis_index("ia") // members
    me_col = lax.axis_index("au")
    lane = lax.broadcasted_iota(jnp.int32, (1, seen.shape[1]), 1)
    col = lax.broadcasted_iota(jnp.int32, (1, mask.shape[1]), 1)
    lines = {r: mask[pl.ds(me_row ^ r, 1), :].astype(f32) * scale for r in sorted(set(rows))}
    for q, rel in enumerate(order):
        for i in range(per):
            here = col == (me_col ^ rel) * per + i
            value = {r: jnp.sum(jnp.where(here, x, 0.0), 1, keepdims=True) for r, x in lines.items()}
            line = None
            for j in reversed(range(len(rows))):
                full = jnp.broadcast_to(value[rows[j]], lane.shape)
                line = full if line is None else jnp.where(lane < (j + 1) * us, full, line)
            seen[pl.ds(q * per + i, 1), :] = line
    for c in copies:
        c.wait()


def load(mask, fac, tan, **static):
    hbm = [pltpu.with_memory_space_constraint(x, pltpu.HBM) for x in (fac, tan)]
    blocks = static["cols_of"][0] * len(static["cols_of"][1])
    lanes = len(static["rows_of"][1]) * static["us"]
    return pl.pallas_call(
        functools.partial(load_kernel, **static),
        in_specs=[VM] + [pl.BlockSpec(memory_space=pltpu.HBM)] * 2,
        out_specs=[VM] * 3,
        out_shape=[pltpu.VMEM(fac.shape, fac.dtype), pltpu.VMEM(tan.shape, tan.dtype), pltpu.VMEM((blocks, lanes), f32)],
        scratch_shapes=[pltpu.SemaphoreType.DMA((2,))],
        compiler_params=PARAMS,
    )(in_vmem(mask), *hbm)


def stack_kernel(a, b, out, sems):
    copies = [
        pltpu.make_async_copy(a, out.at[0, 0], sems.at[0]),
        pltpu.make_async_copy(b, out.at[0, 1], sems.at[1]),
    ]
    for c in copies:
        c.start()
    for c in copies:
        c.wait()


def stack(a, b):
    return pl.pallas_call(
        stack_kernel,
        in_specs=[pl.BlockSpec(memory_space=pltpu.HBM)] * 2,
        out_specs=VM,
        out_shape=pltpu.VMEM((1, 2, *a.shape), a.dtype),
        scratch_shapes=[pltpu.SemaphoreType.DMA((2,))],
        compiler_params=PARAMS,
    )(*[pltpu.with_memory_space_constraint(x, pltpu.HBM) for x in (a, b)])


GROUPS = 8
STEP = 16


def encode_rows(x, out_ref, k):
    rows = x.shape[0]
    groups = min(GROUPS, rows // STEP)
    step = rows // groups
    exps = []
    for g in range(groups):
        part = x[g * step : (g + 1) * step]
        top = jnp.max(jnp.abs(part), 0, keepdims=True)
        e = 14.0 - jnp.ceil(jnp.log2(jnp.maximum(top, 1e-30)))
        out_ref[k, pl.ds(g * step, step), :] = jnp.round(part * jnp.exp2(e)).astype(jnp.int32).astype(jnp.int16)
        exps.append(e)
    exps += exps[-1:] * (GROUPS - groups)
    out_ref[k, pl.ds(rows, GROUPS), :] = jnp.concatenate(exps, 0).astype(jnp.int32).astype(jnp.int16)


def decode_rows(q_ref, k, g, groups):
    rows = q_ref.shape[1] - GROUPS
    step = rows // groups
    unit = jnp.exp2(-q_ref[k, pl.ds(rows, GROUPS), :].astype(jnp.int32).astype(f32))
    return q_ref[k, pl.ds(g * step, step), :].astype(jnp.int32).astype(f32) * unit[g : g + 1]


def encode_kernel(x_ref, out_ref):
    for k in range(x_ref.shape[0]):
        encode_rows(x_ref[k], out_ref, k)


def encode(x):
    n, rows, width = x.shape
    return pl.pallas_call(
        encode_kernel,
        in_specs=[VM],
        out_specs=VM,
        out_shape=pltpu.VMEM((n, rows + GROUPS, width), jnp.int16),
        compiler_params=PARAMS,
    )(in_vmem(x))


def decode_kernel(x_ref, q_ref, out_ref, buf, sems, *, at):
    n, rows, _ = x_ref.shape
    groups = min(GROUPS, rows // STEP)
    step = rows // groups
    parts = sems.shape[1]
    copies = []
    for k in range(n):
        for g in range(groups):
            part = pl.ds(g * step, step)
            buf[k, part, :] = x_ref[k, part, :] + decode_rows(q_ref, at + k, g, groups)
            if (g + 1) % (groups // parts) == 0:
                c = g // (groups // parts)
                done = pl.ds(c * (rows // parts), rows // parts)
                copies.append(pltpu.make_async_copy(buf.at[k, done], out_ref.at[k, done], sems.at[k, c]))
                copies[-1].start()
    for c in copies:
        c.wait()


def add_decoded(x, q, at):
    return pl.pallas_call(
        functools.partial(decode_kernel, at=at),
        in_specs=[VM, VM],
        out_specs=pl.BlockSpec(memory_space=pltpu.HBM),
        out_shape=jax.ShapeDtypeStruct(x.shape, f32),
        scratch_shapes=[pltpu.VMEM(x.shape, f32), pltpu.SemaphoreType.DMA((x.shape[0], 4))],
        compiler_params=PARAMS,
    )(in_vmem(x), in_vmem(q))


def decoded(q_ref, k):
    rows = q_ref.shape[1] - GROUPS
    groups = min(GROUPS, rows // STEP)
    return jnp.concatenate([decode_rows(q_ref, k, g, groups) for g in range(groups)], 0)


def fold_kernel(mine, core_in, coded):
    n, n_a, us, width = core_in.shape
    encode_rows((mine[:n] + core_in[...]).reshape(n * n_a * us, width), coded, 0)


def fold(mine, core_in):
    n, n_a, us, width = core_in.shape
    return pl.pallas_call(
        fold_kernel,
        in_specs=[VM, VM],
        out_specs=VM,
        out_shape=pltpu.VMEM((1, n * n_a * us + GROUPS, width), jnp.int16),
        compiler_params=PARAMS,
    )(in_vmem(mine), in_vmem(core_in))


def spread_kernel(mine, core_in, q, own, *coded):
    n, n_a, us, width = core_in.shape
    rows = n_a * us
    half = rows // 2
    came = decoded(q, 0)
    for i in range(n):
        x = (mine[n + i] + core_in[i]).reshape(rows, width) + came[i * rows : (i + 1) * rows]
        for j in range(2):
            part = x[j * half : (j + 1) * half]
            if i == 0 and j == 0:
                own[...] = part
            else:
                encode_rows(part, coded[2 * i + j - 1], 0)


def spread(mine, core_in, q):
    _, n_a, us, width = core_in.shape
    half = n_a * us // 2
    return pl.pallas_call(
        spread_kernel,
        in_specs=[VM] * 3,
        out_specs=[VM] * 4,
        out_shape=[pltpu.VMEM((half, width), f32)] + [pltpu.VMEM((1, half + GROUPS, width), jnp.int16)] * 3,
        compiler_params=PARAMS,
    )(in_vmem(mine), in_vmem(core_in), in_vmem(q))


def total_kernel(own, *refs):
    x = own[...]
    for q in refs[:-1]:
        x = x + decoded(q, 0)
    refs[-1][...] = x


def total(own, coded):
    return pl.pallas_call(
        total_kernel,
        in_specs=[VM] * (1 + len(coded)),
        out_specs=VM,
        out_shape=jax.ShapeDtypeStruct(own.shape, f32),
        compiler_params=PARAMS,
    )(*[in_vmem(x) for x in (own, *coded)])


def on_device(user_factors, item_factors, user_tangent, item_tangent, block_mask, n_au, n_ia):
    us, width = user_factors.shape
    row_blocks, per = block_mask.shape
    per //= n_au
    members = us * n_ia // row_blocks // us
    assert members == 4
    scale = 1.0 / math.sqrt(width)
    core, near = 1, [0, 2, 4, 6]
    a_bits = bits_of(8, n_ia)
    rel_a = relative(a_bits)

    far = stack(user_factors, user_tangent)
    for bit in a_bits:
        far = jnp.concatenate([far, swap(far, "ia", n_ia, bit)], 0)

    item_bits = bits_of(1, n_au)
    rel_items = relative(item_bits)
    facs, tans = [item_factors[None]], [item_tangent[None]]
    for n, bit in enumerate(item_bits):
        held_f = facs[0] if n == 0 else jnp.concatenate(facs, 0)
        held_t = tans[0] if n == 0 else jnp.concatenate(tans, 0)
        facs.append(swap(held_f, "au", n_au, bit))
        tans.append(swap(held_t, "au", n_au, bit))
    rows = [(b ^ r) // members for b in [*near, near[1], near[3], near[0], near[2]] for r in rel_a]
    facs[0], tans[0], seen = load(
        block_mask, facs[0], tans[0], rows_of=(members, rows), cols_of=(per, rel_items), us=us, scale=scale
    )
    piece = len(rel_a) * us

    mine = [far] + [swap(far, "ia", n_ia, b) for b in near[1:]]
    other = [swap(x, "ia", n_ia, core) for x in mine]

    def call(users, g, sums, sums_at, item_sum, lanes=0, **extra):
        at = sum(f.shape[0] for f in facs[:g])
        return region(
            seen, users, (facs[g], tans[g]), sums, sums_at, item_sum, lanes=lanes, cols=(at, per), scale=scale, **extra
        )

    first, item_sum = call([mine[0], other[0]], 0, [], None, None)
    second, item_sum = call([mine[1], other[1], mine[2], other[2]], 0, [], None, item_sum)
    third, own_items = call([mine[3], other[3]], 0, [], None, item_sum, lanes=2 * piece)
    sums = [first, second, third]
    at_mine, at_other = [(0, 0), (1, 0), (1, 2), (2, 0)], [(0, 1), (1, 1), (1, 3), (2, 1)]
    item_sums = [own_items]
    turn = [1, 3, 0, 2]
    mine, other = [mine[i] for i in turn], [other[i] for i in turn]
    at_mine, at_other = [at_mine[i] for i in turn], [at_other[i] for i in turn]
    for g in range(1, len(facs)):
        first, second = {}, {}
        if facs[g].shape[0] == 1:
            ready = prepare(seen, [*other, *mine], facs[g], lanes=4 * piece, cols=(g, per), scale=scale)
            first = {"ready": ready, "prepared": 0}
            second = {"ready": ready, "prepared": ready[0].shape[0] // 2}
        out_other, item_sum = call(other, g, sums, at_other, None, lanes=4 * piece, **first)
        out_mine, item_sum = call(mine, g, sums, at_mine, item_sum, lanes=4 * piece, **second)
        item_sums.append(item_sum)
        sums = [out_mine, out_other]
        at_mine, at_other = [(0, i) for i in range(4)], [(1, i) for i in range(4)]

    come = [swap(out_other[2 * i : 2 * i + 2], "ia", n_ia, core) for i in range(2)]
    odd = fold(out_mine, come[0])
    own, *coded = spread(out_mine, come[1], swap(odd, "ia", n_ia, near[1]))
    far_bit = a_bits[-1]
    coded = [swap(q, "ia", n_ia, b) for q, b in zip(coded, [far_bit, near[2], far_bit ^ near[2]])]
    acc = total(own, coded)
    for bit in a_bits[:-1][::-1]:
        half = acc.shape[0] // 2
        acc = acc[:half] + swap(acc[half:], "ia", n_ia, bit)
    user_product = acc.reshape(us, width)

    for bit in item_bits[::-1]:
        back = swap(encode(item_sums.pop()), "au", n_au, bit)
        sizes = [h.shape[0] for h in item_sums]
        cuts = [sum(sizes[:i]) for i in range(len(sizes))]
        item_sums = [add_decoded(h, back, c) for h, c in zip(item_sums, cuts)]
    item_product = item_sums[0][0]
    return user_product, item_product


def solution(mesh):
    n_au, n_ia = mesh.shape["au"], mesh.shape["ia"]
    placed = (
        P(("au", "ia"), None),
        P(("ia", "au"), None),
        P(("au", "ia"), None),
        P(("ia", "au"), None),
        P("au", "ia"),
    )

    def body(*args):
        return on_device(*args, n_au=n_au, n_ia=n_ia)

    return jax.shard_map(
        body,
        mesh=mesh,
        in_specs=placed,
        out_specs=(P(("au", "ia"), None), P(("ia", "au"), None)),
        check_vma=False,
    )
```
